256 devices in a mesh: dp: 64 (over y, x, z_lo, core), seq: 4 (over z_hi).
Axes of the slice: x: 4, y: 4, z: 8 (z_hi: 4, z_lo: 2; z = z_hi * 2 + z_lo), core: 2. Of those that a mesh axis runs over, the one named last changes fastest.
Arguments:
- latents: bfloat16 [64, 512, 1536], P('dp', 'seq'), may hold values from -6 to 6
- fresh_noise: bfloat16 [64, 512, 1536], P('dp', 'seq'), may hold values from -6 to 6
- cache_key: bfloat16 [64, 1024, 1536], P('dp', 'seq'), may hold values from -200 to 200, as said below
- cache_value: bfloat16 [64, 1024, 1536], P('dp', 'seq'), may hold values from -6 to 6
- cache_frame: int32 [64, 1024], P('dp', 'seq'), may hold values from 0 to 11
- block_index: int32 [1], replicated, may hold values from 2 to 4
- timestep: int32 [64], P('dp'), may hold values from 20 to 979
- gain_gen: float32 [1536], replicated, may hold values from 0.25 to 1.75
- w_qkv: bfloat16 [1536, 4608], P(None, 'seq'), may hold values from -0.15625 to 0.15625
- w_out: bfloat16 [1536, 1536], P('seq'), may hold values from -0.5 to 0.5
- gain_real: float32 [1536], replicated, may hold values from 0.25 to 1.75
- w_real: bfloat16 [1536, 1536], P(None, 'seq'), may hold values from -0.15625 to 0.15625
- gain_fake: float32 [1536], replicated, may hold values from 0.25 to 1.75
- w_fake: bfloat16 [1536, 1536], P(None, 'seq'), may hold values from -0.15625 to 0.15625
Outputs:
- clean_block: bfloat16 [64, 512, 1536], P('dp', 'seq')
- grad_qkv: float32 [1536, 4608], P('dp', 'seq')
- grad_out: float32 [1536, 1536], P('seq', 'dp')
The draws below stay inside these ranges and needn't reach their ends.
Inputs may be any that keep to these rules, and one draw needn't show every extreme that they name: `cache_key`: cache keys are finite.
All inputs are finite; a program needn't handle non-finite values. Where the reference program divides by a largest or mean magnitude, that divisor is 1e-20 or more.
Results may differ from the reference program's by a relative error of at most 0.02.
The reference program's roundings to bfloat16 on the way count: a program that leaves them out, or rounds other values in their place, can miss the bound.
Values may be sent and summed in bfloat16 or wider, within the bound.
No kernel may reach another device: no remote copies, remote signals or barrier semaphores. Data moves between devices by JAX's collectives and lax.ppermute only.
A program may use at most 128 MiB of HBM per device.

```python
import math
import jax
import jax.numpy as jnp
from jax import lax

HEADS = 12
HEAD_DIM = 128
D = 1536
FRAMES = 3
WINDOW_FRAMES = 6
BATCH = 64
S = 512
L = 1024


def draw_cache_key(key, part):
    base = jax.random.normal(jax.random.fold_in(key, 11), (BATCH, L, D), jnp.float32)
    return jnp.clip(base, -200.0, 200.0).astype(jnp.bfloat16)


def touch_ends(result, own_key, low, top_value):
    longest = result.shape.index(max(result.shape))
    spots = []
    for shift in (0, 1):
        where = [jax.random.randint(jax.random.fold_in(own_key, axis), (), 0, length) for axis, length in enumerate(result.shape)]
        where[longest] = (where[longest] + shift) % result.shape[longest]
        spots.append(tuple(where))
    return result.at[spots[0]].set(low).at[spots[1]].set(top_value)


def shard_levels(stream_key, dims, cuts, smallest, high):
    factor_of = 1.0
    for dim, parts in cuts:
        draws = jax.random.uniform(jax.random.fold_in(jax.random.fold_in(stream_key, 6), dim), (parts,), jnp.float32, smallest / len(cuts), high / len(cuts))
        factor_of = factor_of * jnp.repeat(jnp.exp(draws), dims[dim] // parts).reshape((-1,) + (1,) * (len(dims) - 1 - dim))
    return factor_of


def centred(key, shape, width, most, pieces=(), kind=jnp.bfloat16):
    entries = width * jax.random.normal(key, shape, jnp.float32)
    if pieces:
        entries = entries * shard_levels(key, shape, pieces, -0.22, 0.18)
    return jnp.clip(entries, -most, most).astype(kind)


def setup_inputs(seed: int = 0) -> dict:
    arg_keys = jax.random.split(jax.random.key(seed), 15)
    latents = centred(arg_keys[0], (BATCH, S, D), 1.0, 6.0, ((0, 64), (1, 4)))
    fresh_noise = centred(arg_keys[1], (BATCH, S, D), 1.0, 6.0, ((0, 64), (1, 4)))
    cache_key = draw_cache_key(jax.random.fold_in(arg_keys[14], 71), 0)
    cache_value = centred(arg_keys[3], (BATCH, L, D), 1.0, 6.0, ((0, 64), (1, 4)))
    cache_frame = touch_ends(jax.random.randint(arg_keys[4], (BATCH, L), 0, 12), jax.random.fold_in(arg_keys[4], 1), 0, 11).astype(jnp.int32)
    block_index = jax.random.randint(arg_keys[5], (1,), 2, 5).astype(jnp.int32)
    timestep = touch_ends(jax.random.randint(arg_keys[6], (BATCH,), 20, 980), jax.random.fold_in(arg_keys[6], 1), 20, 979).astype(jnp.int32)
    gain_gen = jnp.clip(1.0 + 0.15 * jax.random.normal(arg_keys[7], (D,), jnp.float32), 0.25, 1.75)
    w_qkv = centred(arg_keys[8], (D, 3 * D), D ** -0.5, 0.15625, ((1, 4),))
    w_out = centred(arg_keys[9], (D, D), HEAD_DIM ** -0.5, 0.5, ((0, 4),))
    gain_real = jnp.clip(1.0 + 0.15 * jax.random.normal(arg_keys[10], (D,), jnp.float32), 0.25, 1.75)
    w_real = centred(arg_keys[11], (D, D), D ** -0.5, 0.15625, ((1, 4),))
    gain_fake = jnp.clip(1.0 + 0.15 * jax.random.normal(arg_keys[12], (D,), jnp.float32), 0.25, 1.75)
    w_fake = centred(arg_keys[13], (D, D), D ** -0.5, 0.15625, ((1, 4),))
    return {"latents": latents, "fresh_noise": fresh_noise, "cache_key": cache_key, "cache_value": cache_value, "cache_frame": cache_frame, "block_index": block_index, "timestep": timestep, "gain_gen": gain_gen, "w_qkv": w_qkv, "w_out": w_out, "gain_real": gain_real, "w_real": w_real, "gain_fake": gain_fake, "w_fake": w_fake}


def norm_rows(values, gain):
    floats = values.astype(jnp.float32)
    return floats * lax.rsqrt(lax.optimization_barrier(jnp.mean(floats * floats, axis=-1, keepdims=True)) + 1e-06) * gain

def attend_forward(query, keys, values, allowed):
    factor = 1.0 / math.sqrt(query.shape[-1])
    scores = jnp.einsum('shd,thd->hst', query.astype(jnp.float32), keys.astype(jnp.float32)) * factor
    scores = jnp.where(allowed[None, None, :], scores, -1e+30)
    top = lax.optimization_barrier(jnp.max(scores, axis=-1, keepdims=True))
    expo = jnp.exp(scores - top)
    probs = expo / lax.optimization_barrier(jnp.sum(expo, axis=-1, keepdims=True))
    weights = probs.astype(jnp.bfloat16)
    mixed = jnp.einsum('hst,thd->shd', weights.astype(jnp.float32), values.astype(jnp.float32)).astype(jnp.bfloat16)
    return (probs, weights, mixed)

def attend_backward(query, keys, values, probs, weights, dmixed, count):
    factor = 1.0 / math.sqrt(query.shape[-1])
    grads = dmixed.astype(jnp.float32)
    dprob = jnp.einsum('shd,thd->hst', grads, values.astype(jnp.float32))
    inner = lax.optimization_barrier(jnp.sum(probs * dprob, axis=-1, keepdims=True))
    dscore = probs * (dprob - inner) * factor
    dquery = jnp.einsum('hst,thd->shd', dscore, keys.astype(jnp.float32))
    dkey = jnp.einsum('hst,shd->thd', dscore[:, :, count:], query.astype(jnp.float32))
    dvalue = jnp.einsum('hst,shd->thd', weights[:, :, count:].astype(jnp.float32), grads)
    return (dquery.astype(jnp.bfloat16), dkey.astype(jnp.bfloat16), dvalue.astype(jnp.bfloat16))

def reference(latents, fresh_noise, cache_key, cache_value, cache_frame, block_index, timestep, gain_gen, w_qkv, w_out, gain_real, w_real, gain_fake, w_fake):
    start = block_index[0] * FRAMES
    length = latents.shape[1]
    span = cache_key.shape[1]

    def sample_step(carry, items):
        tokens, fresh, ckey, cvalue, frames, level = items
        normed = norm_rows(tokens, gain_gen).astype(jnp.bfloat16)
        packed = jnp.dot(normed, w_qkv, preferred_element_type=jnp.float32).astype(jnp.bfloat16)
        packed = packed.reshape(length, HEADS, 3, HEAD_DIM)
        query = packed[:, :, 0]
        keys = jnp.concatenate([ckey.reshape(span, HEADS, HEAD_DIM), packed[:, :, 1]], axis=0)
        values = jnp.concatenate([cvalue.reshape(span, HEADS, HEAD_DIM), packed[:, :, 2]], axis=0)
        allowed = jnp.concatenate([(frames >= start - WINDOW_FRAMES) & (frames < start), jnp.ones((length,), bool)])
        probs, weights, mixed = attend_forward(query, keys, values, allowed)
        flat = mixed.reshape(length, D)
        update = jnp.dot(flat, w_out, preferred_element_type=jnp.float32)
        clean = (tokens.astype(jnp.float32) + update).astype(jnp.bfloat16)
        angle = math.pi / 2 * level.astype(jnp.float32) / 1000.0
        noisy = (jnp.cos(angle) * clean.astype(jnp.float32) + jnp.sin(angle) * fresh.astype(jnp.float32)).astype(jnp.bfloat16)
        pred_real = noisy.astype(jnp.float32) + jnp.dot(norm_rows(noisy, gain_real).astype(jnp.bfloat16), w_real, preferred_element_type=jnp.float32)
        pred_fake = noisy.astype(jnp.float32) + jnp.dot(norm_rows(noisy, gain_fake).astype(jnp.bfloat16), w_fake, preferred_element_type=jnp.float32)
        scale = jnp.mean(jnp.abs(clean.astype(jnp.float32) - pred_real)) + 1e-06
        gap = ((pred_fake - pred_real) / scale).astype(jnp.bfloat16)
        out_grad = jnp.dot(flat.T, gap, preferred_element_type=jnp.float32)
        dmixed = jnp.dot(gap, w_out.T, preferred_element_type=jnp.float32).astype(jnp.bfloat16)
        dmixed = dmixed.reshape(length, HEADS, HEAD_DIM)
        dquery, dkey, dvalue = attend_backward(query, keys, values, probs, weights, dmixed, span)
        dpacked = jnp.stack([dquery, dkey, dvalue], axis=2).reshape(length, 3 * D)
        qkv_grad = jnp.dot(normed.T, dpacked, preferred_element_type=jnp.float32)
        return ((carry[0] + qkv_grad, carry[1] + out_grad), clean)
    start_carry = (jnp.zeros((D, 3 * D), jnp.float32), jnp.zeros((D, D), jnp.float32))
    totals, clean_block = lax.scan(sample_step, start_carry, (latents, fresh_noise, cache_key, cache_value, cache_frame, timestep))
    return (clean_block, totals[0], totals[1])
```

```python
import math

import jax
import jax.numpy as jnp
import numpy as np
from jax import lax
from jax.sharding import PartitionSpec as P

HEAD_DIM = 128
FRAMES = 3
WINDOW_FRAMES = 6
SEQ = 4


def shifted(x, by):
    return lax.ppermute(x, "seq", [(i, (i + by) % SEQ) for i in range(SEQ)])


def plane_groups():
    index = np.arange(64).reshape(4, 4, 2, 2)
    return index.transpose(2, 0, 1, 3).reshape(2, 32).tolist()


def rolled(x, blocks, axis):
    width = x.shape[axis] // SEQ
    lead = ((SEQ - blocks) % SEQ) * width
    return lax.dynamic_slice_in_dim(jnp.concatenate([x, x], axis=axis), lead, x.shape[axis], axis)


def block_of(x, block, axis):
    width = x.shape[axis] // SEQ
    return lax.dynamic_slice_in_dim(x, (block % SEQ) * width, width, axis)


def norm_rows(values, gain):
    floats = values.astype(jnp.float32)
    return floats * lax.rsqrt(jnp.mean(floats * floats, axis=-1, keepdims=True) + 1e-06) * gain


def attend_forward(query, keys, values, allowed):
    factor = 1.0 / math.sqrt(query.shape[-1])
    scores = jnp.einsum("shd,thd->hst", query, keys, preferred_element_type=jnp.float32) * factor
    scores = jnp.where(allowed[None, None, :], scores, -1e30)
    top = jnp.max(scores, axis=-1, keepdims=True)
    expo = jnp.exp(scores - top)
    probs = expo / jnp.sum(expo, axis=-1, keepdims=True)
    weights = probs.astype(jnp.bfloat16)
    mixed = jnp.einsum("hst,thd->shd", weights, values, preferred_element_type=jnp.float32)
    return (probs, weights, mixed.astype(jnp.bfloat16))


def attend_backward(query, keys, values, probs, weights, dmixed, count, unit):
    factor = 1.0 / math.sqrt(query.shape[-1])
    dprob = jnp.einsum("sd,td->st", dmixed, values, preferred_element_type=jnp.float32)
    inner = jnp.sum(probs * dprob, axis=-1, keepdims=True)
    dscore = (probs * (dprob - inner) * (factor * unit)).astype(jnp.bfloat16)
    dquery = jnp.einsum("st,td->sd", dscore, keys, preferred_element_type=jnp.float32)
    dkey = jnp.einsum("st,sd->td", dscore[:, count:], query, preferred_element_type=jnp.float32)
    dvalue = unit * jnp.einsum(
        "st,sd->td", weights[:, count:], dmixed, preferred_element_type=jnp.float32
    )
    return (dquery.astype(jnp.bfloat16), dkey.astype(jnp.bfloat16), dvalue.astype(jnp.bfloat16))


def summed_over_dp(x):
    pieces = x.reshape(64, x.shape[0] // 64, x.shape[1])
    arrived = lax.all_to_all(pieces, "dp", split_axis=0, concat_axis=0, tiled=True)
    return arrived.astype(jnp.float32).sum(axis=0)


def shards(
    latents,
    fresh_noise,
    cache_key,
    cache_value,
    cache_frame,
    block_index,
    timestep,
    gain_gen,
    w_qkv,
    w_out,
    gain_real,
    w_real,
    gain_fake,
    w_fake,
):
    position = lax.axis_index("seq")
    replica = lax.axis_index("dp")
    latents, fresh_noise = latents[0], fresh_noise[0]
    cache_key, cache_value = cache_key[0], cache_value[0]
    count, width = latents.shape
    slots = cache_key.shape[0]
    features = w_out.shape[0]
    heads_here = features // HEAD_DIM

    rows = width // 32
    lead = ((replica // 4) * 2 + replica % 2) * rows
    own = jnp.stack(
        [
            lax.dynamic_slice_in_dim(w_out, lead, rows, 1).T,
            lax.dynamic_slice_in_dim(w_real, lead, rows, 0),
            lax.dynamic_slice_in_dim(w_fake, lead, rows, 0),
        ]
    )
    slices = jnp.concatenate([own] + [shifted(own, -k) for k in range(1, SEQ)], axis=2)
    whole = lax.all_gather(
        rolled(slices, position, 2), "dp", axis=1, tiled=True, axis_index_groups=plane_groups()
    )
    out_t, real, fake = whole[0], whole[1], whole[2]

    tokens = jnp.concatenate([latents] + [shifted(latents, k) for k in range(1, SEQ)], axis=0)
    start = block_index[0] * FRAMES
    open_slots = (cache_frame >= start - WINDOW_FRAMES) & (cache_frame < start)
    flags = jnp.pad(open_slots.astype(jnp.bfloat16), ((0, 7), (0, features - slots)))

    def exchanged(make):
        return [make(position)] + [shifted(make(position + k), k) for k in range(1, SEQ)]

    key_parts = exchanged(lambda j: jnp.concatenate([block_of(cache_key, j, 1), flags], axis=0))
    value_parts = exchanged(lambda j: block_of(cache_value, j, 1))
    normed = norm_rows(tokens, gain_gen).astype(jnp.bfloat16)
    packed = jnp.dot(normed, w_qkv, preferred_element_type=jnp.float32).astype(jnp.bfloat16)
    length = packed.shape[0]
    packed = packed.reshape(length, heads_here, 3, HEAD_DIM)
    query = packed[:, :, 0]
    span = slots * SEQ
    keys = jnp.concatenate(
        [p[:slots].reshape(slots, heads_here, HEAD_DIM) for p in key_parts] + [packed[:, :, 1]]
    )
    values = jnp.concatenate(
        [p.reshape(slots, heads_here, HEAD_DIM) for p in value_parts] + [packed[:, :, 2]]
    )
    allowed = jnp.concatenate([p[slots, :slots] > 0 for p in key_parts] + [jnp.ones((length,), bool)])
    probs, weights, attended = attend_forward(query, keys, values, allowed)
    mixed = attended.reshape(length, features)

    back = [mixed[:count]] + [
        shifted(mixed[k * count : (k + 1) * count], -k) for k in range(1, SEQ)
    ]
    mixed_own = rolled(jnp.concatenate(back, axis=1), position, 1)
    update = jnp.einsum("sk,ek->se", mixed_own, out_t, preferred_element_type=jnp.float32)
    clean = (latents.astype(jnp.float32) + update).astype(jnp.bfloat16)
    angle = math.pi / 2 * timestep.astype(jnp.float32)[0] / 1000.0
    noisy = (
        jnp.cos(angle) * clean.astype(jnp.float32) + jnp.sin(angle) * fresh_noise.astype(jnp.float32)
    ).astype(jnp.bfloat16)
    noisy_f = noisy.astype(jnp.float32)
    pred_real = noisy_f + jnp.dot(
        norm_rows(noisy, gain_real).astype(jnp.bfloat16), real, preferred_element_type=jnp.float32
    )
    pred_fake = noisy_f + jnp.dot(
        norm_rows(noisy, gain_fake).astype(jnp.bfloat16), fake, preferred_element_type=jnp.float32
    )
    partial_sum = jnp.sum(jnp.abs(clean.astype(jnp.float32) - pred_real)).reshape(1, 1)
    gap = (pred_fake - pred_real).astype(jnp.bfloat16)
    dmixed_own = jnp.dot(gap, out_t, preferred_element_type=jnp.float32).astype(jnp.bfloat16)
    dmixed = jnp.concatenate(exchanged(lambda j: block_of(dmixed_own, j, 1)), axis=0)
    total = partial_sum + sum(shifted(partial_sum, k) for k in range(1, SEQ))
    scale = total / (length * width) + 1e-06
    unit = 1.0 / scale
    gap_all = jnp.concatenate([gap] + [shifted(gap, k) for k in range(1, SEQ)], axis=0)

    shares = []
    for head in range(heads_here):
        at = slice(head * HEAD_DIM, (head + 1) * HEAD_DIM)
        grads = attend_backward(
            query[:, head], keys[:, head], values[:, head], probs[head], weights[head],
            dmixed[:, at], span, unit,
        )
        stacked = jnp.concatenate(grads, axis=1)
        shares.append(
            summed_over_dp(
                jnp.einsum("sd,se->de", normed, stacked, preferred_element_type=jnp.float32).astype(
                    jnp.bfloat16
                )
            )
        )
    out_grad = jnp.einsum("se,sk->ek", gap_all, mixed, preferred_element_type=jnp.float32)
    out_share = summed_over_dp((out_grad * unit).astype(jnp.bfloat16)).T
    return (clean[None], jnp.concatenate(shares, axis=1), out_share)


def solution(mesh):
    in_specs = (
        P("dp", "seq", None),
        P("dp", "seq", None),
        P("dp", "seq", None),
        P("dp", "seq", None),
        P("dp", "seq"),
        P(),
        P("dp"),
        P(),
        P(None, "seq"),
        P("seq", None),
        P(),
        P(None, "seq"),
        P(),
        P(None, "seq"),
    )
    out_specs = (P("dp", "seq", None), P("dp", "seq"), P("seq", "dp"))
    return jax.shard_map(shards, mesh=mesh, in_specs=in_specs, out_specs=out_specs, check_vma=False)
```

```python
import math

import jax
import jax.numpy as jnp
import numpy as np
from jax import lax
from jax.experimental import pallas as pl
from jax.experimental.pallas import tpu as pltpu
from jax.sharding import PartitionSpec as P

HEAD_DIM = 128
FRAMES = 3
WINDOW_FRAMES = 6
SEQ = 4
PARTS = 64


def shifted(x, by):
    return lax.ppermute(x, "seq", [(i, (i + by) % SEQ) for i in range(SEQ)])


def plane_groups():
    index = np.arange(64).reshape(4, 4, 2, 2)
    return index.transpose(2, 0, 1, 3).reshape(2, 32).tolist()


def chip_groups():
    return np.arange(PARTS).reshape(-1, 2).T.tolist()


def block_of(x, block, axis):
    width = x.shape[axis] // SEQ
    return lax.dynamic_slice_in_dim(x, (block % SEQ) * width, width, axis)


def dot(a, b, contract=((1,), (0,))):
    return lax.dot_general(a, b, (contract, ((), ())), preferred_element_type=jnp.float32)


NT = ((1,), (1,))
TN = ((0,), (0,))
VMEM = pl.BlockSpec(memory_space=pltpu.VMEM)
SMEM = pl.BlockSpec(memory_space=pltpu.SMEM)
ANY = pl.BlockSpec(memory_space=pl.ANY)
PARAMS = pltpu.CompilerParams(vmem_limit_bytes=56 * 1024 * 1024)


def out(shape, dtype=jnp.bfloat16):
    return jax.ShapeDtypeStruct(shape, dtype)


def normed_rows(values, gain):
    floats = values.astype(jnp.float32)
    return floats * lax.rsqrt(jnp.mean(floats * floats, axis=-1, keepdims=True) + 1e-06) * gain


def slices_kernel(at_ref, a_ref, b_ref, c_ref, o_ref):
    o_ref[0] = a_ref[...]
    o_ref[1] = b_ref[...]
    o_ref[2] = c_ref[...]


def weight_slices(a, b, c, at, rows):
    spec = pl.BlockSpec((rows, a.shape[1]), lambda i, at: (at[0], 0))
    return pl.pallas_call(
        slices_kernel,
        grid_spec=pltpu.PrefetchScalarGridSpec(
            num_scalar_prefetch=1,
            grid=(1,),
            in_specs=[spec] * 3,
            out_specs=pl.BlockSpec((3, rows, a.shape[1]), lambda i, at: (0, 0, 0)),
        ),
        out_shape=out((3, rows, a.shape[1])),
        name="weight_slices",
    )(at, a, b, c)


def place_kernel(at_ref, *refs):
    o_ref = refs[-1]
    width = refs[0].shape[2]
    for k in range(SEQ):
        lead = pl.multiple_of(((at_ref[0] + k) % SEQ) * width, 128)
        o_ref[:, :, pl.ds(lead, width)] = refs[k][...]


def placed(parts, at):
    n, rows, width = parts[0].shape
    return pl.pallas_call(
        place_kernel,
        in_specs=[SMEM] + [VMEM] * SEQ,
        out_specs=VMEM,
        out_shape=out((n, rows, width * SEQ)),
        name="placed",
    )(at, *parts)


def project_kernel(*refs):
    parts, (gain_ref, w_ref, normed_ref, packed_ref) = refs[:SEQ], refs[SEQ:]
    count = parts[0].shape[0]
    for k in range(SEQ):
        normed_ref[k * count : (k + 1) * count] = normed_rows(parts[k][...], gain_ref[...]).astype(
            jnp.bfloat16
        )
    packed_ref[...] = dot(normed_ref[...], w_ref[...]).astype(jnp.bfloat16)


def project(parts, gain, w):
    length = parts[0].shape[0] * SEQ
    return pl.pallas_call(
        project_kernel,
        in_specs=[VMEM] * (SEQ + 2),
        out_specs=[VMEM] * 2,
        out_shape=[out((length, w.shape[0])), out((length, w.shape[1]))],
        compiler_params=PARAMS,
        name="project",
    )(*parts, gain.reshape(1, -1), w)


def weights_kernel(*refs):
    parts, (q_ref, k_ref, o_ref) = refs[:SEQ], refs[SEQ:]
    factor = 1.0 / math.sqrt(HEAD_DIM)
    slots = parts[0].shape[0] - 8
    span = slots * SEQ
    keys = [p[:slots] for p in parts] + [k_ref[...]]
    flags = [
        jnp.concatenate([p[slots + r : slots + r + 1] for r in range(slots // HEAD_DIM)], axis=1)
        > 0.5
        for p in parts
    ]
    step = 128
    for r in range(q_ref.shape[0] // step):
        rows = slice(r * step, (r + 1) * step)
        query = q_ref[rows]
        scores = [dot(query, k, NT) * factor for k in keys]
        for n in range(SEQ):
            scores[n] = jnp.where(flags[n], scores[n], -1e30)
        top = jnp.max(scores[SEQ], axis=-1, keepdims=True)
        for n in range(SEQ):
            top = jnp.maximum(top, jnp.max(scores[n], axis=-1, keepdims=True))
        expo = [jnp.exp(s - top) for s in scores]
        total = sum(jnp.sum(e, axis=-1, keepdims=True) for e in expo)
        over = 1.0 / total
        for n in range(SEQ):
            o_ref[0, rows, n * slots : (n + 1) * slots] = (expo[n] * over).astype(jnp.bfloat16)
        o_ref[0, rows, span:] = (expo[SEQ] * over).astype(jnp.bfloat16)


def attention_weights(key_parts, packed):
    length = packed.shape[0]
    heads = key_parts[0].shape[1] // HEAD_DIM
    rows = key_parts[0].shape[0]
    total = (rows - 8) * SEQ + length
    part = pl.BlockSpec((rows, HEAD_DIM), lambda h: (0, h))
    return pl.pallas_call(
        weights_kernel,
        grid=(heads,),
        in_specs=[part] * SEQ
        + [pl.BlockSpec((length, HEAD_DIM), lambda h, j=j: (0, 3 * h + j)) for j in range(2)],
        out_specs=pl.BlockSpec((1, length, total), lambda h: (h, 0, 0)),
        out_shape=out((heads, length, total)),
        compiler_params=PARAMS,
        name="attention_weights",
    )(*key_parts, packed, packed)


def mix_kernel(*refs):
    w_ref, parts, v_ref, outs = refs[0], refs[1 : SEQ + 1], refs[SEQ + 1], refs[SEQ + 2 :]
    slots = parts[0].shape[0]
    count = outs[0].shape[0]
    mixed = dot(w_ref[0, :, slots * SEQ :], v_ref[...])
    for n in range(SEQ):
        mixed += dot(w_ref[0, :, n * slots : (n + 1) * slots], parts[n][...])
    mixed = mixed.astype(jnp.bfloat16)
    for n in range(SEQ):
        outs[n][...] = mixed[n * count : (n + 1) * count]


def attention_mix(weights, value_parts, packed):
    heads, length, total = weights.shape
    slots, features = value_parts[0].shape
    count = length // SEQ
    return pl.pallas_call(
        mix_kernel,
        grid=(heads,),
        in_specs=[pl.BlockSpec((1, length, total), lambda h: (h, 0, 0))]
        + [pl.BlockSpec((slots, HEAD_DIM), lambda h: (0, h))] * SEQ
        + [pl.BlockSpec((length, HEAD_DIM), lambda h: (0, 3 * h + 2))],
        out_specs=[pl.BlockSpec((count, HEAD_DIM), lambda h: (0, h))] * SEQ,
        out_shape=[out((count, features))] * SEQ,
        compiler_params=PARAMS,
        name="attention_mix",
    )(weights, *value_parts, packed)


def middle_kernel(*refs):
    at_ref, blend_ref = refs[:2]
    parts, refs = refs[2 : SEQ + 2], refs[SEQ + 2 :]
    latents_ref, fresh_ref, real_gain_ref, fake_gain_ref, w_ref = refs[:5]
    clean_ref, gap_ref, sum_ref = refs[5:8]
    outs, (held, sems) = refs[8 : 8 + SEQ], refs[8 + SEQ :]
    copies = [pltpu.make_async_copy(w_ref.at[n], held.at[n], sems.at[n]) for n in range(3)]
    for c in copies:
        c.start()
    width = parts[0].shape[1]

    def block(k):
        lead = pl.multiple_of(((at_ref[0] + k) % SEQ) * width, 128)
        return held[0, :, pl.ds(lead, width)]

    copies[0].wait()
    update = dot(parts[0][...], block(0), NT)
    for k in range(1, SEQ):
        update += dot(parts[k][...], block(k), NT)
    clean = (latents_ref[...].astype(jnp.float32) + update).astype(jnp.bfloat16)
    clean_ref[...] = clean
    clean_f = clean.astype(jnp.float32)
    noisy = (
        (blend_ref[0] * clean_f + blend_ref[1] * fresh_ref[...].astype(jnp.float32))
        .astype(jnp.bfloat16)
        .astype(jnp.float32)
    )
    scaled = noisy * lax.rsqrt(jnp.mean(noisy * noisy, axis=-1, keepdims=True) + 1e-06)
    real_in = (scaled * real_gain_ref[...]).astype(jnp.bfloat16)
    fake_in = (scaled * fake_gain_ref[...]).astype(jnp.bfloat16)
    copies[1].wait()
    pred_real = noisy + dot(real_in, held[1])
    sum_ref[...] = jnp.broadcast_to(
        jnp.sum(jnp.abs(clean_f - pred_real), axis=(0, 1), keepdims=True), sum_ref.shape
    )
    copies[2].wait()
    pred_fake = noisy + dot(fake_in, held[2])
    gap = (pred_fake - pred_real).astype(jnp.bfloat16)
    gap_ref[...] = gap
    for k in range(SEQ):
        outs[k][...] = dot(gap, block(k)).astype(jnp.bfloat16)


def middle(at, blend, parts, latents, fresh, gain_real, gain_fake, whole):
    count, width = latents.shape
    return pl.pallas_call(
        middle_kernel,
        in_specs=[SMEM] * 2 + [VMEM] * (SEQ + 4) + [ANY],
        out_specs=[VMEM] * (3 + SEQ),
        out_shape=[out((count, width)), out((count, width)), out((8, 128), jnp.float32)]
        + [out(parts[0].shape)] * SEQ,
        scratch_shapes=[pltpu.VMEM(whole.shape, jnp.bfloat16), pltpu.SemaphoreType.DMA((3,))],
        compiler_params=PARAMS,
        name="middle",
    )(at, blend, *parts, latents, fresh, gain_real.reshape(1, -1), gain_fake.reshape(1, -1), whole)


def split_rows(held, core, send_ref, keep_ref):
    pairs = PARTS // 2
    rows = held.shape[0] // PARTS
    for n in range(pairs):
        at = slice(n * rows, (n + 1) * rows)
        send_ref[at] = held[pl.ds(pl.multiple_of((2 * n + 1 - core) * rows, 8), rows)].astype(
            jnp.bfloat16
        )
        keep_ref[at] = held[pl.ds(pl.multiple_of((2 * n + core) * rows, 8), rows)].astype(
            jnp.bfloat16
        )


def backward_kernel(*refs):
    core_ref, unit_ref, w_ref, normed_ref = refs[:4]
    grads, refs = refs[4 : SEQ + 4], refs[SEQ + 4 :]
    key_parts, value_parts, refs = refs[:SEQ], refs[SEQ : 2 * SEQ], refs[2 * SEQ :]
    q_ref, k_ref, v_ref, send_ref, keep_ref, dpacked, held = refs
    unit = unit_ref[0]
    factor = 1.0 / math.sqrt(HEAD_DIM) * unit
    slots = value_parts[0].shape[0]
    span = slots * SEQ
    keys = [p[:slots] for p in key_parts] + [k_ref[...]]
    values = [p[...] for p in value_parts] + [v_ref[...]]
    count = grads[0].shape[0]
    dkey = jnp.zeros(k_ref.shape, jnp.float32)
    dvalue = jnp.zeros(k_ref.shape, jnp.float32)
    for r in range(SEQ):
        rows = slice(r * count, (r + 1) * count)
        dmixed = grads[r][...]
        weights = [w_ref[0, rows, n * slots : (n + 1) * slots] for n in range(SEQ)]
        weights.append(w_ref[0, rows, span:])
        probs = [w.astype(jnp.float32) for w in weights]
        dprobs = [dot(dmixed, v, NT) for v in values]
        inner = sum(jnp.sum(p * d, axis=-1, keepdims=True) for p, d in zip(probs, dprobs))
        dscores = [
            (p * (d - inner) * factor).astype(jnp.bfloat16) for p, d in zip(probs, dprobs)
        ]
        dquery = sum(dot(d, k) for d, k in zip(dscores, keys))
        dpacked[rows, :HEAD_DIM] = dquery.astype(jnp.bfloat16)
        dkey += dot(dscores[SEQ], q_ref[rows], TN)
        dvalue += dot(weights[SEQ], dmixed, TN)
    dpacked[:, HEAD_DIM : 2 * HEAD_DIM] = dkey.astype(jnp.bfloat16)
    dpacked[:, 2 * HEAD_DIM :] = (dvalue * unit).astype(jnp.bfloat16)
    held[...] = dot(normed_ref[...], dpacked[...], TN)
    split_rows(held, core_ref[0], send_ref, keep_ref)


def backward(core, unit, weights, normed, grads, key_parts, value_parts, packed):
    heads, length, total = weights.shape
    width = normed.shape[1]
    slots = value_parts[0].shape[0]
    part = lambda rows: pl.BlockSpec((rows, HEAD_DIM), lambda h: (0, h))
    half = pl.BlockSpec((width // 2, 3 * HEAD_DIM), lambda h: (0, h))
    return pl.pallas_call(
        backward_kernel,
        grid=(heads,),
        in_specs=[SMEM] * 2
        + [pl.BlockSpec((1, length, total), lambda h: (h, 0, 0))]
        + [pl.BlockSpec((length, width), lambda h: (0, 0))]
        + [part(grads[0].shape[0])] * SEQ
        + [part(key_parts[0].shape[0])] * SEQ
        + [part(slots)] * SEQ
        + [pl.BlockSpec((length, HEAD_DIM), lambda h, j=j: (0, 3 * h + j)) for j in range(3)],
        out_specs=[half] * 2,
        out_shape=[out((width // 2, packed.shape[1]))] * 2,
        scratch_shapes=[
            pltpu.VMEM((length, 3 * HEAD_DIM), jnp.bfloat16),
            pltpu.VMEM((width, 3 * HEAD_DIM), jnp.float32),
        ],
        compiler_params=PARAMS,
        name="backward",
    )(core, unit, weights, normed, *grads, *key_parts, *value_parts, packed, packed, packed)


def out_grad_kernel(*refs):
    core_ref, unit_ref = refs[:2]
    gaps, mixed, (send_ref, keep_ref, held) = refs[2 : SEQ + 2], refs[SEQ + 2 : 2 * SEQ + 2], refs[2 * SEQ + 2 :]
    total = dot(gaps[0][...], mixed[0][...], TN)
    for k in range(1, SEQ):
        total += dot(gaps[k][...], mixed[k][...], TN)
    held[...] = total * unit_ref[0]
    split_rows(held, core_ref[0], send_ref, keep_ref)


def out_gradient(core, unit, gaps, mixed):
    width, features = gaps[0].shape[1], mixed[0].shape[1]
    return pl.pallas_call(
        out_grad_kernel,
        in_specs=[SMEM] * 2 + [VMEM] * (2 * SEQ),
        out_specs=[VMEM] * 2,
        out_shape=[out((width // 2, features))] * 2,
        scratch_shapes=[pltpu.VMEM((width, features), jnp.float32)],
        compiler_params=PARAMS,
        name="out_gradient",
    )(core, unit, *gaps, *mixed)


def chip_sum(send, keep):
    arrived = lax.ppermute(send, "dp", [(i, i ^ 1) for i in range(PARTS)])
    return (keep.astype(jnp.float32) + arrived.astype(jnp.float32)).astype(jnp.bfloat16)


def summed_over_chips(x):
    pieces = x.reshape(PARTS // 2, x.shape[0] * 2 // PARTS, x.shape[1])
    arrived = lax.all_to_all(
        pieces, "dp", split_axis=0, concat_axis=0, tiled=True, axis_index_groups=chip_groups()
    )
    return arrived.astype(jnp.float32).sum(axis=0)


def shards(
    latents,
    fresh_noise,
    cache_key,
    cache_value,
    cache_frame,
    block_index,
    timestep,
    gain_gen,
    w_qkv,
    w_out,
    gain_real,
    w_real,
    gain_fake,
    w_fake,
):
    position = lax.axis_index("seq")
    replica = lax.axis_index("dp")
    latents, fresh_noise = latents[0], fresh_noise[0]
    cache_key, cache_value = cache_key[0], cache_value[0]
    count, width = latents.shape
    slots = cache_key.shape[0]
    features = w_out.shape[0]
    heads_here = features // HEAD_DIM

    at = jnp.reshape(position, (1,)).astype(jnp.int32)
    core = jnp.reshape(replica % 2, (1,)).astype(jnp.int32)
    slice_at = jnp.reshape((replica // 4) * 2 + replica % 2, (1,)).astype(jnp.int32)
    own = weight_slices(w_out.T, w_real, w_fake, slice_at, width // (PARTS // 2))
    slices = placed([own] + [shifted(own, -k) for k in range(1, SEQ)], at)
    whole = lax.all_gather(slices, "dp", axis=1, tiled=True, axis_index_groups=plane_groups())

    tokens = [latents] + [shifted(latents, k) for k in range(1, SEQ)]
    start = block_index[0] * FRAMES
    open_slots = (cache_frame >= start - WINDOW_FRAMES) & (cache_frame < start)
    flags = open_slots.astype(jnp.bfloat16).reshape(slots // HEAD_DIM, HEAD_DIM)
    flags = jnp.pad(jnp.tile(flags, (1, heads_here)), ((0, 8 - slots // HEAD_DIM), (0, 0)))

    def exchanged(make):
        return [make(position)] + [shifted(make(position + k), k) for k in range(1, SEQ)]

    key_parts = exchanged(lambda j: jnp.concatenate([block_of(cache_key, j, 1), flags], axis=0))
    value_parts = exchanged(lambda j: block_of(cache_value, j, 1))
    normed, packed = project(tokens, gain_gen, w_qkv)
    length = packed.shape[0]
    weights = attention_weights(key_parts, packed)
    mixed = attention_mix(weights, value_parts, packed)

    back = [mixed[0]] + [shifted(mixed[k], -k) for k in range(1, SEQ)]
    angle = math.pi / 2 * timestep.astype(jnp.float32) / 1000.0
    blend = jnp.concatenate([jnp.cos(angle), jnp.sin(angle)])
    clean, gap, partial_sum, *dmixed = middle(
        at, blend, back, latents, fresh_noise, gain_real, gain_fake, whole
    )
    grads = [dmixed[0]] + [shifted(dmixed[k], k) for k in range(1, SEQ)]
    total = partial_sum + sum(shifted(partial_sum, k) for k in range(1, SEQ))
    unit = 1.0 / (total[0, :1] / (length * width) + 1e-06)
    gaps = [gap] + [shifted(gap, k) for k in range(1, SEQ)]
    qkv_share = summed_over_chips(
        chip_sum(*backward(core, unit, weights, normed, grads, key_parts, value_parts, packed))
    )
    out_share = summed_over_chips(chip_sum(*out_gradient(core, unit, gaps, mixed))).T
    return (clean[None], qkv_share, out_share)


def solution(mesh):
    in_specs = (
        P("dp", "seq", None),
        P("dp", "seq", None),
        P("dp", "seq", None),
        P("dp", "seq", None),
        P("dp", "seq"),
        P(),
        P("dp"),
        P(),
        P(None, "seq"),
        P("seq", None),
        P(),
        P(None, "seq"),
        P(),
        P(None, "seq"),
    )
    out_specs = (P("dp", "seq", None), P("dp", "seq"), P("seq", "dp"))
    return jax.shard_map(shards, mesh=mesh, in_specs=in_specs, out_specs=out_specs, check_vma=False)
```

```python
import math

import jax
import jax.numpy as jnp
import numpy as np
from jax import lax
from jax.experimental import pallas as pl
from jax.experimental.pallas import tpu as pltpu
from jax.sharding import PartitionSpec as P


HEAD_DIM = 128
FRAMES = 3
WINDOW_FRAMES = 6
SEQ = 4
PARTS = 64


def shifted(x, by):
    return lax.ppermute(x, "seq", [(i, (i + by) % SEQ) for i in range(SEQ)])


def plane_groups():
    index = np.arange(64).reshape(4, 4, 2, 2)
    return index.transpose(2, 0, 1, 3).reshape(2, 32).tolist()


def chip_groups():
    return np.arange(PARTS).reshape(-1, 2).T.tolist()


def block_of(x, block, axis):
    width = x.shape[axis] // SEQ
    return lax.dynamic_slice_in_dim(x, (block % SEQ) * width, width, axis)


def dot(a, b, contract=((1,), (0,))):
    return lax.dot_general(a, b, (contract, ((), ())), preferred_element_type=jnp.float32)


NT = ((1,), (1,))
TN = ((0,), (0,))
VMEM = pl.BlockSpec(memory_space=pltpu.VMEM)
SMEM = pl.BlockSpec(memory_space=pltpu.SMEM)
ANY = pl.BlockSpec(memory_space=pl.ANY)


def near(*arrays):
    return [pltpu.with_memory_space_constraint(a, pltpu.VMEM) for a in arrays]


def far(*arrays):
    return [pltpu.with_memory_space_constraint(a, pltpu.HBM) for a in arrays]


def far_out(shape):
    return pltpu.HBM(shape, jnp.bfloat16)


def near_out(shape):
    return pltpu.VMEM(shape, jnp.bfloat16)


def within(mebibytes):
    return pltpu.CompilerParams(vmem_limit_bytes=mebibytes * 1024 * 1024)


def place_in_seq(k):
    return lax.rem(lax.axis_index("seq") + k, SEQ)


def normed_rows(values, gain):
    floats = values.astype(jnp.float32)
    return floats * lax.rsqrt(jnp.mean(floats * floats, axis=-1, keepdims=True) + 1e-06) * gain


def slices_kernel(at_ref, a_ref, b_ref, c_ref, o_ref):
    o_ref[0] = a_ref[...]
    o_ref[1] = b_ref[...]
    o_ref[2] = c_ref[...]


def weight_slices(a, b, c, at, rows):
    spec = pl.BlockSpec((rows, a.shape[1]), lambda i, at: (at[0], 0))
    return pl.pallas_call(
        slices_kernel,
        grid_spec=pltpu.PrefetchScalarGridSpec(
            num_scalar_prefetch=1,
            grid=(1,),
            in_specs=[spec] * 3,
            out_specs=pl.BlockSpec((3, rows, a.shape[1]), lambda i, at: (0, 0, 0)),
        ),
        out_shape=far_out((3, rows, a.shape[1])),
        name="weight_slices",
    )(at, *far(a, b, c))


def place_kernel(*refs):
    o_ref = refs[-1]
    width = refs[0].shape[2]
    for k in range(SEQ):
        lead = pl.multiple_of(place_in_seq(k) * width, 128)
        o_ref[:, :, pl.ds(lead, width)] = refs[k][...]


def placed(parts):
    n, rows, width = parts[0].shape
    return pl.pallas_call(
        place_kernel,
        in_specs=[VMEM] * SEQ,
        out_specs=VMEM,
        out_shape=far_out((n, rows, width * SEQ)),
        compiler_params=within(4),
        name="placed",
    )(*far(*parts))


def project_kernel(*refs):
    parts, (gain_ref, w_ref, turned_ref, packed_ref, held) = refs[:-5], refs[-5:]
    row = 0
    for part in parts:
        at = slice(row, row + part.shape[0])
        row += part.shape[0]
        held[at] = normed_rows(part[...], gain_ref[...]).astype(jnp.bfloat16)
    count = parts[0].shape[0]
    for k in range(SEQ):
        at = slice(k * count, (k + 1) * count)
        turned_ref[:, at] = held[at].T
    packed_ref[...] = dot(held[...], w_ref[...]).astype(jnp.bfloat16)


def project(parts, gain, w):
    length = parts[0].shape[0] * SEQ
    return pl.pallas_call(
        project_kernel,
        in_specs=[VMEM] * (len(parts) + 2),
        out_specs=[VMEM] * 2,
        out_shape=[near_out((w.shape[0], length)), near_out((length, w.shape[1]))],
        scratch_shapes=[pltpu.VMEM((length, w.shape[0]), jnp.bfloat16)],
        compiler_params=within(24),
        name="project",
    )(*far(parts[0]), *far(*parts[1:]), *far(gain.reshape(1, -1), w))


def weights_kernel(*refs):
    parts, (q_ref, k_ref, o_ref) = refs[:SEQ], refs[SEQ:]
    factor = 1.0 / math.sqrt(HEAD_DIM)
    slots = parts[0].shape[0] - 8
    span = slots * SEQ
    keys = [p[:slots] for p in parts] + [k_ref[...]]
    flags = [
        jnp.concatenate([p[slots + r : slots + r + 1] for r in range(slots // HEAD_DIM)], axis=1)
        > 0.5
        for p in parts
    ]
    step = 128
    for r in range(q_ref.shape[0] // step):
        rows = slice(r * step, (r + 1) * step)
        query = q_ref[rows]
        scores = [dot(query, k, NT) * factor for k in keys]
        for n in range(SEQ):
            scores[n] = jnp.where(flags[n], scores[n], -1e30)
        top = jnp.max(scores[SEQ], axis=-1, keepdims=True)
        for n in range(SEQ):
            top = jnp.maximum(top, jnp.max(scores[n], axis=-1, keepdims=True))
        expo = [jnp.exp(s - top) for s in scores]
        total = sum(jnp.sum(e, axis=-1, keepdims=True) for e in expo)
        over = 1.0 / total
        for n in range(SEQ):
            o_ref[0, rows, n * slots : (n + 1) * slots] = (expo[n] * over).astype(jnp.bfloat16)
        o_ref[0, rows, span:] = (expo[SEQ] * over).astype(jnp.bfloat16)


def attention_weights(key_parts, packed):
    length = packed.shape[0]
    heads = key_parts[0].shape[1] // HEAD_DIM
    rows = key_parts[0].shape[0]
    total = (rows - 8) * SEQ + length
    part = pl.BlockSpec((rows, HEAD_DIM), lambda h: (0, h))
    return pl.pallas_call(
        weights_kernel,
        grid=(heads,),
        in_specs=[part] * SEQ
        + [pl.BlockSpec((length, HEAD_DIM), lambda h, j=j: (0, 3 * h + j)) for j in range(2)],
        out_specs=pl.BlockSpec((1, length, total), lambda h: (h, 0, 0)),
        out_shape=near_out((heads, length, total)),
        compiler_params=within(20),
        name="attention_weights",
    )(*far(*key_parts), *near(packed, packed))


def mix_kernel(*refs):
    w_ref, parts, v_ref, outs = refs[0], refs[1 : SEQ + 1], refs[SEQ + 1], refs[SEQ + 2 :]
    slots = parts[0].shape[0]
    count = outs[0].shape[0]
    mixed = dot(w_ref[0, :, slots * SEQ :], v_ref[...])
    for n in range(SEQ):
        mixed += dot(w_ref[0, :, n * slots : (n + 1) * slots], parts[n][...])
    mixed = mixed.astype(jnp.bfloat16)
    for n in range(SEQ):
        outs[n][...] = mixed[n * count : (n + 1) * count]


def attention_mix(weights, value_parts, packed):
    heads, length, total = weights.shape
    slots, features = value_parts[0].shape
    count = length // SEQ
    return pl.pallas_call(
        mix_kernel,
        grid=(heads,),
        in_specs=[pl.BlockSpec((1, length, total), lambda h: (h, 0, 0))]
        + [pl.BlockSpec((slots, HEAD_DIM), lambda h: (0, h))] * SEQ
        + [pl.BlockSpec((length, HEAD_DIM), lambda h: (0, 3 * h + 2))],
        out_specs=[pl.BlockSpec((count, HEAD_DIM), lambda h: (0, h))] * SEQ,
        out_shape=[far_out((count, features))] * SEQ,
        compiler_params=within(12),
        name="attention_mix",
    )(*near(weights), *far(*value_parts), *near(packed))


def in_terms(total, shape):
    row = lax.broadcasted_iota(jnp.int32, shape, 0)
    result = jnp.zeros(shape, jnp.float32)
    for n in range(3):
        term = total.astype(jnp.bfloat16).astype(jnp.float32)
        result = jnp.where(row == n, term, result)
        total = total - term
    return result.astype(jnp.bfloat16)


def unit_of(grads, entries):
    total = sum(g[-8:, :HEAD_DIM].astype(jnp.float32) for g in grads)
    total = jnp.sum(total, axis=0, keepdims=True)[:, :1]
    return 1.0 / (total / entries + 1e-06)


def middle_kernel(*refs):
    parts, refs = refs[:SEQ], refs[SEQ:]
    blend_ref, latents_ref, fresh_ref, real_gain_ref, fake_gain_ref, w_ref = refs[:6]
    clean_ref, gap_ref = refs[6:8]
    outs, (held, sems) = refs[8 : 8 + SEQ], refs[8 + SEQ :]
    copies = [pltpu.make_async_copy(w_ref.at[n], held.at[n], sems.at[n]) for n in range(3)]
    for c in copies:
        c.start()
    width = parts[0].shape[1]

    def block(k):
        lead = pl.multiple_of(place_in_seq(k) * width, 128)
        return held[0, :, pl.ds(lead, width)]

    copies[0].wait()
    update = dot(parts[0][...], block(0), NT)
    for k in range(1, SEQ):
        update += dot(parts[k][...], block(k), NT)
    clean = (latents_ref[...].astype(jnp.float32) + update).astype(jnp.bfloat16)
    clean_ref[...] = clean
    clean_f = clean.astype(jnp.float32)
    noisy = (
        (blend_ref[0:1, 0:1] * clean_f + blend_ref[1:2, 0:1] * fresh_ref[...].astype(jnp.float32))
        .astype(jnp.bfloat16)
        .astype(jnp.float32)
    )
    scaled = noisy * lax.rsqrt(jnp.mean(noisy * noisy, axis=-1, keepdims=True) + 1e-06)
    real_in = (scaled * real_gain_ref[...]).astype(jnp.bfloat16)
    fake_in = (scaled * fake_gain_ref[...]).astype(jnp.bfloat16)
    copies[1].wait()
    pred_real = noisy + dot(real_in, held[1])
    total = jnp.sum(jnp.abs(clean_f - pred_real), axis=(0, 1), keepdims=True)
    copies[2].wait()
    pred_fake = noisy + dot(fake_in, held[2])
    gap = (pred_fake - pred_real).astype(jnp.bfloat16)
    gap_ref[...] = gap
    count = gap.shape[0]
    terms = in_terms(total, (8, width))
    for k in range(SEQ):
        outs[k][:count] = dot(gap, block(k)).astype(jnp.bfloat16)
        outs[k][count:] = terms


def middle(blend, parts, latents, fresh, gain_real, gain_fake, whole):
    count, width = latents.shape
    return pl.pallas_call(
        middle_kernel,
        in_specs=[VMEM] * (SEQ + 5) + [ANY],
        out_specs=[VMEM] * (2 + SEQ),
        out_shape=[far_out((count, width))] * 2
        + [near_out((count + 8, parts[0].shape[1]))] * SEQ,
        scratch_shapes=[pltpu.VMEM(whole.shape, jnp.bfloat16), pltpu.SemaphoreType.DMA((3,))],
        compiler_params=within(30),
        name="middle",
    )(
        *far(*parts, blend, latents, fresh, gain_real.reshape(1, -1), gain_fake.reshape(1, -1)),
        *far(whole),
    )


def split_rows(held, send_ref, keep_ref):
    core = lax.rem(lax.axis_index("dp"), 2)
    pairs = PARTS // 2
    rows = held.shape[0] // PARTS
    for n in range(pairs):
        at = slice(n * rows, (n + 1) * rows)
        send_ref[at] = held[pl.ds(pl.multiple_of((2 * n + 1 - core) * rows, 8), rows)].astype(
            jnp.bfloat16
        )
        keep_ref[at] = held[pl.ds(pl.multiple_of((2 * n + core) * rows, 8), rows)].astype(
            jnp.bfloat16
        )


def backward_kernel(*refs):
    w_ref, turned_ref = refs[:2]
    grads, refs = refs[2 : SEQ + 2], refs[SEQ + 2 :]
    key_parts, value_parts, refs = refs[:SEQ], refs[SEQ : 2 * SEQ], refs[2 * SEQ :]
    q_ref, k_ref, v_ref, send_ref, keep_ref, dpacked, held = refs
    length, width = dpacked.shape[0], turned_ref.shape[0]
    unit = unit_of(grads, length * width)
    factor = 1.0 / math.sqrt(HEAD_DIM) * unit
    slots = value_parts[0].shape[0]
    span = slots * SEQ
    keys = [p[:slots] for p in key_parts] + [k_ref[...]]
    values = [p[...] for p in value_parts] + [v_ref[...]]
    count = length // SEQ
    dkey = jnp.zeros((HEAD_DIM, length), jnp.float32)
    dvalue = jnp.zeros((HEAD_DIM, length), jnp.float32)
    per = 2
    for r in range(SEQ // per):
        rows = slice(r * per * count, (r + 1) * per * count)
        dmixed = jnp.concatenate([g[:count] for g in grads[r * per : (r + 1) * per]], axis=0)
        weights = [w_ref[0, rows, n * slots : (n + 1) * slots] for n in range(SEQ)]
        weights.append(w_ref[0, rows, span:])
        dprobs = [dot(dmixed, v, NT) for v in values]
        inner = sum(
            jnp.sum(p.astype(jnp.float32) * d, axis=-1, keepdims=True)
            for p, d in zip(weights, dprobs)
        )
        dscores = [
            (p.astype(jnp.float32) * (d - inner) * factor).astype(jnp.bfloat16)
            for p, d in zip(weights, dprobs)
        ]
        dquery = sum(dot(d, k) for d, k in zip(dscores, keys))
        dpacked[rows, :HEAD_DIM] = dquery.astype(jnp.bfloat16)
        dkey += dot(q_ref[rows], dscores[SEQ], TN)
        dvalue += dot(dmixed, weights[SEQ], TN)
    dpacked[:, HEAD_DIM : 2 * HEAD_DIM] = dkey.astype(jnp.bfloat16).T
    dpacked[:, 2 * HEAD_DIM :] = (dvalue * unit).astype(jnp.bfloat16).T
    held[...] = dot(turned_ref[...], dpacked[...])
    split_rows(held, send_ref, keep_ref)


def backward(weights, turned, grads, key_parts, value_parts, packed):
    heads, length, total = weights.shape
    width = turned.shape[0]
    slots = value_parts[0].shape[0]
    part = lambda rows: pl.BlockSpec((rows, HEAD_DIM), lambda h: (0, h))
    half = pl.BlockSpec((width // 2, 3 * HEAD_DIM), lambda h: (0, h))
    return pl.pallas_call(
        backward_kernel,
        grid=(heads,),
        in_specs=[pl.BlockSpec((1, length, total), lambda h: (h, 0, 0))]
        + [pl.BlockSpec((width, length), lambda h: (0, 0))]
        + [part(grads[0].shape[0])] * SEQ
        + [part(key_parts[0].shape[0])] * SEQ
        + [part(slots)] * SEQ
        + [pl.BlockSpec((length, HEAD_DIM), lambda h, j=j: (0, 3 * h + j)) for j in range(3)],
        out_specs=[half] * 2,
        out_shape=[far_out((width // 2, packed.shape[1]))] * 2,
        scratch_shapes=[
            pltpu.VMEM((length, 3 * HEAD_DIM), jnp.bfloat16),
            pltpu.VMEM((width, 3 * HEAD_DIM), jnp.float32),
        ],
        compiler_params=within(26),
        name="backward",
    )(
        *near(weights, turned, *grads),
        *far(*key_parts, *value_parts),
        *near(packed, packed, packed),
    )


def out_grad_kernel(*refs):
    grads, gaps, mixed = refs[:SEQ], refs[SEQ : 2 * SEQ], refs[2 * SEQ : 3 * SEQ]
    send_ref, keep_ref, held = refs[3 * SEQ :]
    total = dot(gaps[0][...], mixed[0][...], TN)
    for k in range(1, SEQ):
        total += dot(gaps[k][...], mixed[k][...], TN)
    entries = gaps[0].shape[0] * SEQ * gaps[0].shape[1]
    held[...] = total * unit_of(grads, entries)
    split_rows(held, send_ref, keep_ref)


def out_gradient(grads, gaps, mixed):
    width, features = gaps[0].shape[1], mixed[0].shape[1]
    return pl.pallas_call(
        out_grad_kernel,
        in_specs=[VMEM] * (3 * SEQ),
        out_specs=[VMEM] * 2,
        out_shape=[far_out((width // 2, features))] * 2,
        scratch_shapes=[pltpu.VMEM((width, features), jnp.float32)],
        compiler_params=within(16),
        name="out_gradient",
    )(*near(*grads), *far(*gaps, *mixed))


def chip_sum(send, keep):
    arrived = lax.ppermute(send, "dp", [(i, i ^ 1) for i in range(PARTS)])
    return (keep.astype(jnp.float32) + arrived.astype(jnp.float32)).astype(jnp.bfloat16)


def summed_over_chips(x):
    pieces = x.reshape(PARTS // 2, x.shape[0] * 2 // PARTS, x.shape[1])
    arrived = lax.all_to_all(
        pieces, "dp", split_axis=0, concat_axis=0, tiled=True, axis_index_groups=chip_groups()
    )
    return arrived.astype(jnp.float32).sum(axis=0)


def shards(
    latents,
    fresh_noise,
    cache_key,
    cache_value,
    cache_frame,
    block_index,
    timestep,
    gain_gen,
    w_qkv,
    w_out,
    gain_real,
    w_real,
    gain_fake,
    w_fake,
):
    position = lax.axis_index("seq")
    replica = lax.axis_index("dp")
    latents, fresh_noise = latents[0], fresh_noise[0]
    cache_key, cache_value = cache_key[0], cache_value[0]
    count, width = latents.shape
    slots = cache_key.shape[0]
    features = w_out.shape[0]
    heads_here = features // HEAD_DIM

    slice_at = jnp.reshape((replica // 4) * 2 + replica % 2, (1,)).astype(jnp.int32)
    own = weight_slices(w_out.T, w_real, w_fake, slice_at, width // (PARTS // 2))
    parts = [own] + [shifted(own, -k) for k in range(1, SEQ)]
    slices = placed(parts)
    whole = lax.all_gather(slices, "dp", axis=1, tiled=True, axis_index_groups=plane_groups())

    half = count // 2
    before, after = shifted(latents, 1), shifted(latents, -1)
    tokens = [latents, before, shifted(before[:half], 1), shifted(after[half:], -1), after]
    start = block_index[0] * FRAMES
    open_slots = (cache_frame >= start - WINDOW_FRAMES) & (cache_frame < start)
    flags = open_slots.astype(jnp.bfloat16).reshape(slots // HEAD_DIM, HEAD_DIM)
    flags = jnp.pad(jnp.tile(flags, (1, heads_here)), ((0, 8 - slots // HEAD_DIM), (0, 0)))

    def exchanged(make):
        return [make(position)] + [shifted(make(position + k), k) for k in range(1, SEQ)]

    key_parts = exchanged(lambda j: jnp.concatenate([block_of(cache_key, j, 1), flags], axis=0))
    value_parts = exchanged(lambda j: block_of(cache_value, j, 1))
    turned, packed = project(tokens, gain_gen, w_qkv)
    weights = attention_weights(key_parts, packed)
    mixed = attention_mix(weights, value_parts, packed)

    back = [mixed[0]] + [shifted(mixed[k], -k) for k in range(1, SEQ)]
    angle = math.pi / 2 * timestep.astype(jnp.float32) / 1000.0
    blend = jnp.broadcast_to(jnp.stack([jnp.cos(angle), jnp.sin(angle)]), (2, HEAD_DIM))
    clean, gap, *dmixed = middle(
        blend, back, latents, fresh_noise, gain_real, gain_fake, whole
    )
    grads = [dmixed[0]] + [shifted(dmixed[k], k) for k in range(1, SEQ)]
    gaps = [gap] + [shifted(gap, k) for k in range(1, SEQ)]
    halves = backward(weights, turned, grads, key_parts, value_parts, packed)
    qkv = chip_sum(*halves)
    halves = out_gradient(grads, gaps, mixed)
    outg = chip_sum(*halves)
    first = 2 * 3 * HEAD_DIM
    share_a = summed_over_chips(qkv[:, :first])
    share_b = summed_over_chips(jnp.concatenate([qkv[:, first:], outg], axis=1))
    rest = qkv.shape[1] - first
    qkv_share = jnp.concatenate([share_a, share_b[:, :rest]], axis=1)
    return (clean[None], qkv_share, share_b[:, rest:].T)


def solution(mesh):
    in_specs = (
        P("dp", "seq", None),
        P("dp", "seq", None),
        P("dp", "seq", None),
        P("dp", "seq", None),
        P("dp", "seq"),
        P(),
        P("dp"),
        P(),
        P(None, "seq"),
        P("seq", None),
        P(),
        P(None, "seq"),
        P(),
        P(None, "seq"),
    )
    out_specs = (P("dp", "seq", None), P("dp", "seq"), P("seq", "dp"))

    return jax.shard_map(shards, mesh=mesh, in_specs=in_specs, out_specs=out_specs, check_vma=False)
```

```python
import math

import jax
import jax.numpy as jnp
import numpy as np
from jax import lax
from jax.experimental import pallas as pl
from jax.experimental.pallas import tpu as pltpu
from jax.sharding import PartitionSpec as P


HEAD_DIM = 128
FRAMES = 3
WINDOW_FRAMES = 6
SEQ = 4
PARTS = 64


def shifted(x, by):
    return lax.ppermute(x, "seq", [(i, (i + by) % SEQ) for i in range(SEQ)])


def plane_groups():
    index = np.arange(64).reshape(4, 4, 2, 2)
    return index.transpose(2, 0, 1, 3).reshape(2, 32).tolist()


def chip_groups():
    return np.arange(PARTS).reshape(-1, 2).T.tolist()


def block_of(x, block, axis):
    width = x.shape[axis] // SEQ
    return lax.dynamic_slice_in_dim(x, (block % SEQ) * width, width, axis)


def dot(a, b, contract=((1,), (0,))):
    return lax.dot_general(a, b, (contract, ((), ())), preferred_element_type=jnp.float32)


NT = ((1,), (1,))
TN = ((0,), (0,))
VMEM = pl.BlockSpec(memory_space=pltpu.VMEM)
SMEM = pl.BlockSpec(memory_space=pltpu.SMEM)
ANY = pl.BlockSpec(memory_space=pl.ANY)


def near(*arrays):
    return [pltpu.with_memory_space_constraint(a, pltpu.VMEM) for a in arrays]


def far(*arrays):
    return [pltpu.with_memory_space_constraint(a, pltpu.HBM) for a in arrays]


def far_out(shape):
    return pltpu.HBM(shape, jnp.bfloat16)


def near_out(shape):
    return pltpu.VMEM(shape, jnp.bfloat16)


def within(mebibytes):
    return pltpu.CompilerParams(vmem_limit_bytes=mebibytes * 1024 * 1024)


def place_in_seq(k):
    return lax.rem(lax.axis_index("seq") + k, SEQ)


def normed_rows(values, gain):
    floats = values.astype(jnp.float32)
    return floats * lax.rsqrt(jnp.mean(floats * floats, axis=-1, keepdims=True) + 1e-06) * gain


def slices_kernel(at_ref, a_ref, b_ref, c_ref, o_ref):
    o_ref[0] = a_ref[...]
    o_ref[1] = b_ref[...]
    o_ref[2] = c_ref[...]


def weight_slices(a, b, c, at, rows):
    width = b.shape[1]
    first = pl.BlockSpec((rows, width), lambda i, at: (at[0] // SEQ, at[0] % SEQ))
    spec = pl.BlockSpec((rows, width), lambda i, at: (at[0], 0))
    return pl.pallas_call(
        slices_kernel,
        grid_spec=pltpu.PrefetchScalarGridSpec(
            num_scalar_prefetch=1,
            grid=(1,),
            in_specs=[first, spec, spec],
            out_specs=pl.BlockSpec((3, rows, width), lambda i, at: (0, 0, 0)),
        ),
        out_shape=far_out((3, rows, width)),
        name="weight_slices",
    )(at, *far(a, b, c))


def place_kernel(*refs):
    o_ref = refs[-1]
    width = refs[0].shape[2]
    for k in range(SEQ):
        lead = pl.multiple_of(place_in_seq(k) * width, 128)
        o_ref[:, :, pl.ds(lead, width)] = refs[k][...]


def placed(parts):
    n, rows, width = parts[0].shape
    return pl.pallas_call(
        place_kernel,
        in_specs=[VMEM] * SEQ,
        out_specs=VMEM,
        out_shape=far_out((n, rows, width * SEQ)),
        compiler_params=within(4),
        name="placed",
    )(*far(*parts))


def project_kernel(*refs):
    parts, (gain_ref, w_ref, turned_ref, packed_ref, held) = refs[:-5], refs[-5:]
    row = 0
    for part in parts:
        at = slice(row, row + part.shape[0])
        row += part.shape[0]
        held[at] = normed_rows(part[...], gain_ref[...]).astype(jnp.bfloat16)
    count = parts[0].shape[0]
    for k in range(SEQ):
        at = slice(k * count, (k + 1) * count)
        turned_ref[:, at] = held[at].T
    packed_ref[...] = dot(held[...], w_ref[...]).astype(jnp.bfloat16)


def project(parts, gain, w):
    length = parts[0].shape[0] * SEQ
    return pl.pallas_call(
        project_kernel,
        in_specs=[VMEM] * (len(parts) + 2),
        out_specs=[VMEM] * 2,
        out_shape=[near_out((w.shape[0], length)), near_out((length, w.shape[1]))],
        scratch_shapes=[pltpu.VMEM((length, w.shape[0]), jnp.bfloat16)],
        compiler_params=within(24),
        name="project",
    )(*far(parts[0]), *far(*parts[1:]), *far(gain.reshape(1, -1), w))


def weights_kernel(*refs):
    parts, (q_ref, k_ref, o_ref) = refs[:SEQ], refs[SEQ:]
    factor = 1.0 / math.sqrt(HEAD_DIM)
    slots = parts[0].shape[0] - 8
    span = slots * SEQ
    keys = [p[:slots] for p in parts] + [k_ref[...]]
    flags = [
        jnp.concatenate([p[slots + r : slots + r + 1] for r in range(slots // HEAD_DIM)], axis=1)
        > 0.5
        for p in parts
    ]
    step = 128

    @pl.loop(0, q_ref.shape[0] // step)
    def _(r):
        rows = pl.ds(pl.multiple_of(r * step, step), step)
        query = q_ref[rows]
        scores = [dot(query, k, NT) * factor for k in keys]
        for n in range(SEQ):
            scores[n] = jnp.where(flags[n], scores[n], -1e30)
        top = jnp.max(scores[SEQ], axis=-1, keepdims=True)
        for n in range(SEQ):
            top = jnp.maximum(top, jnp.max(scores[n], axis=-1, keepdims=True))
        expo = [jnp.exp(s - top) for s in scores]
        total = sum(jnp.sum(e, axis=-1, keepdims=True) for e in expo)
        over = 1.0 / total
        for n in range(SEQ):
            o_ref[0, rows, n * slots : (n + 1) * slots] = (expo[n] * over).astype(jnp.bfloat16)
        o_ref[0, rows, span:] = (expo[SEQ] * over).astype(jnp.bfloat16)


def attention_weights(key_parts, packed):
    length = packed.shape[0]
    heads = key_parts[0].shape[1] // HEAD_DIM
    rows = key_parts[0].shape[0]
    total = (rows - 8) * SEQ + length
    part = pl.BlockSpec((rows, HEAD_DIM), lambda h: (0, h))
    return pl.pallas_call(
        weights_kernel,
        grid=(heads,),
        in_specs=[part] * SEQ
        + [pl.BlockSpec((length, HEAD_DIM), lambda h, j=j: (0, 3 * h + j)) for j in range(2)],
        out_specs=pl.BlockSpec((1, length, total), lambda h: (h, 0, 0)),
        out_shape=near_out((heads, length, total)),
        compiler_params=within(20),
        name="attention_weights",
    )(*far(*key_parts), *near(packed, packed))


def mix_kernel(*refs):
    w_ref, parts, v_ref, outs = refs[0], refs[1 : SEQ + 1], refs[SEQ + 1], refs[SEQ + 2 :]
    slots = parts[0].shape[0]
    count = outs[0].shape[0]
    mixed = dot(w_ref[0, :, slots * SEQ :], v_ref[...])
    for n in range(SEQ):
        mixed += dot(w_ref[0, :, n * slots : (n + 1) * slots], parts[n][...])
    mixed = mixed.astype(jnp.bfloat16)
    for n in range(SEQ):
        outs[n][...] = mixed[n * count : (n + 1) * count]


def attention_mix(weights, value_parts, packed):
    heads, length, total = weights.shape
    slots, features = value_parts[0].shape
    count = length // SEQ
    return pl.pallas_call(
        mix_kernel,
        grid=(heads,),
        in_specs=[pl.BlockSpec((1, length, total), lambda h: (h, 0, 0))]
        + [pl.BlockSpec((slots, HEAD_DIM), lambda h: (0, h))] * SEQ
        + [pl.BlockSpec((length, HEAD_DIM), lambda h: (0, 3 * h + 2))],
        out_specs=[pl.BlockSpec((count, HEAD_DIM), lambda h: (0, h))] * SEQ,
        out_shape=[far_out((count, features))] * SEQ,
        compiler_params=within(12),
        name="attention_mix",
    )(*near(weights), *far(*value_parts), *near(packed))


def in_terms(total, shape):
    row = lax.broadcasted_iota(jnp.int32, shape, 0)
    result = jnp.zeros(shape, jnp.float32)
    for n in range(3):
        term = total.astype(jnp.bfloat16).astype(jnp.float32)
        result = jnp.where(row == n, term, result)
        total = total - term
    return result.astype(jnp.bfloat16)


def unit_of(grads, entries):
    total = sum(g[-8:, :HEAD_DIM].astype(jnp.float32) for g in grads)
    total = jnp.sum(total, axis=0, keepdims=True)[:, :1]
    return 1.0 / (total / entries + 1e-06)


def middle_kernel(*refs):
    parts, refs = refs[:SEQ], refs[SEQ:]
    blend_ref, latents_ref, fresh_ref, real_gain_ref, fake_gain_ref, w_ref = refs[:6]
    clean_ref, gap_ref = refs[6:8]
    outs, (out_w, held, sems) = refs[8 : 8 + SEQ], refs[8 + SEQ :]
    width = parts[0].shape[1]

    @pl.loop(0, SEQ)
    def _(j):
        for c in range(SEQ):
            pltpu.make_async_copy(
                w_ref.at[0, :, c, :, pl.ds(pl.multiple_of(j * width, 128), width)],
                out_w.at[j, :, :, c * width : (c + 1) * width],
                sems.at[0],
            ).start()

    copies = [pltpu.make_async_copy(out_w, out_w, sems.at[0])]
    for n in (1, 2):
        copies.append(pltpu.make_async_copy(w_ref.at[n], held.at[n - 1], sems.at[n]))
        copies[n].start()

    def block(k):
        rows = out_w[place_in_seq(k)]
        return rows.reshape(width, rows.shape[2])

    copies[0].wait()
    update = dot(parts[0][...], block(0))
    for k in range(1, SEQ):
        update += dot(parts[k][...], block(k))
    clean = (latents_ref[...].astype(jnp.float32) + update).astype(jnp.bfloat16)
    clean_ref[...] = clean
    clean_f = clean.astype(jnp.float32)
    noisy = (
        (blend_ref[0:1, 0:1] * clean_f + blend_ref[1:2, 0:1] * fresh_ref[...].astype(jnp.float32))
        .astype(jnp.bfloat16)
        .astype(jnp.float32)
    )
    scaled = noisy * lax.rsqrt(jnp.mean(noisy * noisy, axis=-1, keepdims=True) + 1e-06)
    gain_shape = (clean.shape[1], clean.shape[1])
    real_in = (scaled * real_gain_ref[...]).astype(jnp.bfloat16)
    fake_in = (scaled * fake_gain_ref[...]).astype(jnp.bfloat16)
    copies[1].wait()
    pred_real = noisy + dot(real_in, held[0].reshape(gain_shape))
    total = jnp.sum(jnp.abs(clean_f - pred_real), axis=(0, 1), keepdims=True)
    copies[2].wait()
    pred_fake = noisy + dot(fake_in, held[1].reshape(gain_shape))
    gap = (pred_fake - pred_real).astype(jnp.bfloat16)
    gap_ref[...] = gap
    count = gap.shape[0]
    terms = in_terms(total, (8, width))
    for k in range(SEQ):
        outs[k][:count] = dot(gap, block(k), NT).astype(jnp.bfloat16)
        outs[k][count:] = terms


def middle(blend, parts, latents, fresh, gain_real, gain_fake, whole):
    count, width = latents.shape
    return pl.pallas_call(
        middle_kernel,
        in_specs=[VMEM] * (SEQ + 5) + [ANY],
        out_specs=[VMEM] * (2 + SEQ),
        out_shape=[far_out((count, width))] * 2
        + [near_out((count + 8, parts[0].shape[1]))] * SEQ,
        scratch_shapes=[
            pltpu.VMEM((SEQ, whole.shape[1], *whole.shape[3:]), jnp.bfloat16),
            pltpu.VMEM((2, *whole.shape[1:]), jnp.bfloat16),
            pltpu.SemaphoreType.DMA((3,)),
        ],
        compiler_params=within(30),
        name="middle",
    )(
        *far(*parts, blend, latents, fresh, gain_real.reshape(1, -1), gain_fake.reshape(1, -1)),
        *far(whole),
    )


def split_rows(held, send_ref, keep_ref):
    core = lax.rem(lax.axis_index("dp"), 2)
    pairs = PARTS // 2
    rows = held.shape[0] // PARTS

    @pl.loop(0, pairs)
    def _(n):
        at = pl.ds(pl.multiple_of(n * rows, 8), rows)
        other, own = (2 * n + 1 - core) * rows, (2 * n + core) * rows
        send_ref[at] = held[pl.ds(pl.multiple_of(other, 8), rows)].astype(jnp.bfloat16)
        keep_ref[at] = held[pl.ds(pl.multiple_of(own, 8), rows)].astype(jnp.bfloat16)


def backward_kernel(*refs):
    w_ref, turned_ref = refs[:2]
    grads, refs = refs[2 : SEQ + 2], refs[SEQ + 2 :]
    key_parts, value_parts, refs = refs[:SEQ], refs[SEQ : 2 * SEQ], refs[2 * SEQ :]
    q_ref, k_ref, v_ref, send_ref, keep_ref, dpacked, held = refs
    length, width = dpacked.shape[0], turned_ref.shape[0]
    unit = unit_of(grads, length * width)
    factor = 1.0 / math.sqrt(HEAD_DIM) * unit
    slots = value_parts[0].shape[0]
    span = slots * SEQ
    keys = [p[:slots] for p in key_parts] + [k_ref[...]]
    values = [p[...] for p in value_parts] + [v_ref[...]]
    count = length // SEQ
    dkey = jnp.zeros((HEAD_DIM, length), jnp.float32)
    dvalue = jnp.zeros((HEAD_DIM, length), jnp.float32)
    per = 2
    for r in range(SEQ // per):
        rows = slice(r * per * count, (r + 1) * per * count)
        dmixed = jnp.concatenate([g[:count] for g in grads[r * per : (r + 1) * per]], axis=0)
        weights = [w_ref[0, rows, n * slots : (n + 1) * slots] for n in range(SEQ)]
        weights.append(w_ref[0, rows, span:])
        dprobs = [dot(dmixed, v, NT) for v in values]
        inner = sum(
            jnp.sum(p.astype(jnp.float32) * d, axis=-1, keepdims=True)
            for p, d in zip(weights, dprobs)
        )
        dscores = [
            (p.astype(jnp.float32) * (d - inner) * factor).astype(jnp.bfloat16)
            for p, d in zip(weights, dprobs)
        ]
        dquery = sum(dot(d, k) for d, k in zip(dscores, keys))
        dpacked[rows, :HEAD_DIM] = dquery.astype(jnp.bfloat16)
        dkey += dot(q_ref[rows], dscores[SEQ], TN)
        dvalue += dot(dmixed, weights[SEQ], TN)
    dpacked[:, HEAD_DIM : 2 * HEAD_DIM] = dkey.astype(jnp.bfloat16).T
    dpacked[:, 2 * HEAD_DIM :] = (dvalue * unit).astype(jnp.bfloat16).T
    held[...] = dot(turned_ref[...], dpacked[...])
    split_rows(held, send_ref, keep_ref)


def backward(first, heads, weights, turned, grads, key_parts, value_parts, packed):
    length, total = weights.shape[1:]
    width = turned.shape[0]
    slots = value_parts[0].shape[0]
    part = lambda rows: pl.BlockSpec((rows, HEAD_DIM), lambda h: (0, first + h))
    half = pl.BlockSpec((width // 2, 3 * HEAD_DIM), lambda h: (0, h))
    return pl.pallas_call(
        backward_kernel,
        grid=(heads,),
        in_specs=[pl.BlockSpec((1, length, total), lambda h: (first + h, 0, 0))]
        + [pl.BlockSpec((width, length), lambda h: (0, 0))]
        + [part(grads[0].shape[0])] * SEQ
        + [part(key_parts[0].shape[0])] * SEQ
        + [part(slots)] * SEQ
        + [pl.BlockSpec((length, HEAD_DIM), lambda h, j=j: (0, 3 * (first + h) + j)) for j in range(3)],
        out_specs=[half] * 2,
        out_shape=[far_out((width // 2, heads * 3 * HEAD_DIM))] * 2,
        scratch_shapes=[
            pltpu.VMEM((length, 3 * HEAD_DIM), jnp.bfloat16),
            pltpu.VMEM((width, 3 * HEAD_DIM), jnp.float32),
        ],
        compiler_params=within(26),
        name="backward",
    )(
        *near(weights, turned, *grads),
        *far(*key_parts, *value_parts),
        *near(packed, packed, packed),
    )


def out_grad_kernel(*refs):
    grads, gaps, mixed = refs[:SEQ], refs[SEQ : 2 * SEQ], refs[2 * SEQ : 3 * SEQ]
    send_ref, keep_ref, held = refs[3 * SEQ :]
    total = dot(gaps[0][...], mixed[0][...], TN)
    for k in range(1, SEQ):
        total += dot(gaps[k][...], mixed[k][...], TN)
    entries = gaps[0].shape[0] * SEQ * gaps[0].shape[1]
    held[...] = total * unit_of(grads, entries)
    split_rows(held, send_ref, keep_ref)


def out_gradient(grads, gaps, mixed):
    width, features = gaps[0].shape[1], mixed[0].shape[1]
    return pl.pallas_call(
        out_grad_kernel,
        in_specs=[VMEM] * (3 * SEQ),
        out_specs=[VMEM] * 2,
        out_shape=[far_out((width // 2, features))] * 2,
        scratch_shapes=[pltpu.VMEM((width, features), jnp.float32)],
        compiler_params=within(16),
        name="out_gradient",
    )(*near(*grads), *far(*gaps, *mixed))


def chip_sum(send, keep):
    arrived = lax.ppermute(send, "dp", [(i, i ^ 1) for i in range(PARTS)])
    return (keep.astype(jnp.float32) + arrived.astype(jnp.float32)).astype(jnp.bfloat16)


def summed_over_chips(x):
    pieces = x.reshape(PARTS // 2, x.shape[0] * 2 // PARTS, x.shape[1])
    arrived = lax.all_to_all(
        pieces, "dp", split_axis=0, concat_axis=0, tiled=True, axis_index_groups=chip_groups()
    )
    return arrived.astype(jnp.float32).sum(axis=0)


def shards(
    latents,
    fresh_noise,
    cache_key,
    cache_value,
    cache_frame,
    block_index,
    timestep,
    gain_gen,
    w_qkv,
    w_out,
    gain_real,
    w_real,
    gain_fake,
    w_fake,
):
    position = lax.axis_index("seq")
    replica = lax.axis_index("dp")
    latents, fresh_noise = latents[0], fresh_noise[0]
    cache_key, cache_value = cache_key[0], cache_value[0]
    count, width = latents.shape
    slots = cache_key.shape[0]
    features = w_out.shape[0]
    heads_here = features // HEAD_DIM

    slice_at = jnp.reshape((replica // 4) * 2 + replica % 2, (1,)).astype(jnp.int32)
    own = weight_slices(w_out, w_real, w_fake, slice_at, width // (PARTS // 2))
    parts = [own] + [shifted(own, -k) for k in range(1, SEQ)]
    slices = placed(parts)
    whole = lax.all_gather(slices, "dp", axis=1, tiled=True, axis_index_groups=plane_groups())
    whole = whole.reshape(3, PARTS // 2 // SEQ, SEQ, slices.shape[1], width)

    half = count // 2
    before, after = shifted(latents, 1), shifted(latents, -1)
    tokens = [latents, before, shifted(before[:half], 1), shifted(after[half:], -1), after]
    start = block_index[0] * FRAMES
    open_slots = (cache_frame >= start - WINDOW_FRAMES) & (cache_frame < start)
    flags = open_slots.astype(jnp.bfloat16).reshape(slots // HEAD_DIM, HEAD_DIM)
    flags = jnp.pad(jnp.tile(flags, (1, heads_here)), ((0, 8 - slots // HEAD_DIM), (0, 0)))

    def exchanged(make):
        return [make(position)] + [shifted(make(position + k), k) for k in range(1, SEQ)]

    key_parts = exchanged(lambda j: jnp.concatenate([block_of(cache_key, j, 1), flags], axis=0))
    value_parts = exchanged(lambda j: block_of(cache_value, j, 1))
    turned, packed = project(tokens, gain_gen, w_qkv)
    weights = attention_weights(key_parts, packed)
    mixed = attention_mix(weights, value_parts, packed)

    back = [mixed[0]] + [shifted(mixed[k], -k) for k in range(1, SEQ)]
    angle = math.pi / 2 * timestep.astype(jnp.float32) / 1000.0
    blend = jnp.broadcast_to(jnp.stack([jnp.cos(angle), jnp.sin(angle)]), (2, HEAD_DIM))
    clean, gap, *dmixed = middle(
        blend, back, latents, fresh_noise, gain_real, gain_fake, whole
    )
    grads = [dmixed[0]] + [shifted(dmixed[k], k) for k in range(1, SEQ)]
    gaps = [gap] + [shifted(gap, k) for k in range(1, SEQ)]
    sums = []
    for heads in (range(0, heads_here - 1), range(heads_here - 1, heads_here)):
        halves = backward(
            heads[0], len(heads), weights, turned, grads, key_parts, value_parts, packed
        )
        sums.append(chip_sum(*halves))
    halves = out_gradient(grads, gaps, mixed)
    outg = chip_sum(*halves)
    share_a = summed_over_chips(sums[0])
    share_b = summed_over_chips(jnp.concatenate([sums[1], outg], axis=1))
    rest = sums[1].shape[1]
    qkv_share = jnp.concatenate([share_a, share_b[:, :rest]], axis=1)
    return (clean[None], qkv_share, share_b[:, rest:].T)


def solution(mesh):
    in_specs = (
        P("dp", "seq", None),
        P("dp", "seq", None),
        P("dp", "seq", None),
        P("dp", "seq", None),
        P("dp", "seq"),
        P(),
        P("dp"),
        P(),
        P(None, "seq"),
        P("seq", None),
        P(),
        P(None, "seq"),
        P(),
        P(None, "seq"),
    )
    out_specs = (P("dp", "seq", None), P("dp", "seq"), P("seq", "dp"))

    return jax.shard_map(shards, mesh=mesh, in_specs=in_specs, out_specs=out_specs, check_vma=False)
```

```python
import math

import jax
import jax.numpy as jnp
import numpy as np
from jax import lax
from jax.experimental import pallas as pl
from jax.experimental.pallas import tpu as pltpu
from jax.sharding import PartitionSpec as P


HEAD_DIM = 128
FRAMES = 3
WINDOW_FRAMES = 6
SEQ = 4
PARTS = 64


def shifted(x, by):
    return lax.ppermute(x, "seq", [(i, (i + by) % SEQ) for i in range(SEQ)])


def plane_groups():
    index = np.arange(64).reshape(4, 4, 2, 2)
    return index.transpose(2, 0, 1, 3).reshape(2, 32).tolist()


def chip_groups():
    return np.arange(PARTS).reshape(-1, 2).T.tolist()


def block_of(x, block, axis):
    width = x.shape[axis] // SEQ
    return lax.dynamic_slice_in_dim(x, (block % SEQ) * width, width, axis)


def dot(a, b, contract=((1,), (0,))):
    return lax.dot_general(a, b, (contract, ((), ())), preferred_element_type=jnp.float32)


NT = ((1,), (1,))
TN = ((0,), (0,))
VMEM = pl.BlockSpec(memory_space=pltpu.VMEM)
SMEM = pl.BlockSpec(memory_space=pltpu.SMEM)
ANY = pl.BlockSpec(memory_space=pl.ANY)


def near(*arrays):
    return [pltpu.with_memory_space_constraint(a, pltpu.VMEM) for a in arrays]


def far(*arrays):
    return [pltpu.with_memory_space_constraint(a, pltpu.HBM) for a in arrays]


def far_out(shape):
    return pltpu.HBM(shape, jnp.bfloat16)


def near_out(shape):
    return pltpu.VMEM(shape, jnp.bfloat16)


def within(mebibytes):
    return pltpu.CompilerParams(vmem_limit_bytes=mebibytes * 1024 * 1024)


def place_in_seq(k):
    return lax.rem(lax.axis_index("seq") + k, SEQ)


def normed_rows(values, gain):
    floats = values.astype(jnp.float32)
    return floats * lax.rsqrt(jnp.mean(floats * floats, axis=-1, keepdims=True) + 1e-06) * gain


def slices_kernel(at_ref, a_ref, b_ref, c_ref, o_ref):
    o_ref[0] = a_ref[...]
    o_ref[1] = b_ref[...]
    o_ref[2] = c_ref[...]


def weight_slices(a, b, c, at, rows):
    width = b.shape[1]
    first = pl.BlockSpec((rows, width), lambda i, at: (at[0] // SEQ, at[0] % SEQ))
    spec = pl.BlockSpec((rows, width), lambda i, at: (at[0], 0))
    return pl.pallas_call(
        slices_kernel,
        grid_spec=pltpu.PrefetchScalarGridSpec(
            num_scalar_prefetch=1,
            grid=(1,),
            in_specs=[first, spec, spec],
            out_specs=pl.BlockSpec((3, rows, width), lambda i, at: (0, 0, 0)),
        ),
        out_shape=far_out((3, rows, width)),
        name="weight_slices",
    )(at, *far(a, b, c))


def place_kernel(*refs):
    o_ref = refs[-1]
    width = refs[0].shape[2]
    for k in range(SEQ):
        lead = pl.multiple_of(place_in_seq(k) * width, 128)
        o_ref[:, :, pl.ds(lead, width)] = refs[k][...]


def placed(parts):
    n, rows, width = parts[0].shape
    return pl.pallas_call(
        place_kernel,
        in_specs=[VMEM] * SEQ,
        out_specs=VMEM,
        out_shape=far_out((n, rows, width * SEQ)),
        compiler_params=within(4),
        name="placed",
    )(*far(*parts))


def project_kernel(*refs):
    parts, (gain_ref, w_ref, turned_ref, packed_ref, held) = refs[:-5], refs[-5:]
    row = 0
    for part in parts:
        at = slice(row, row + part.shape[0])
        row += part.shape[0]
        held[at] = normed_rows(part[...], gain_ref[...]).astype(jnp.bfloat16)
    count = parts[0].shape[0]
    for k in range(SEQ):
        at = slice(k * count, (k + 1) * count)
        turned_ref[:, at] = held[at].T
    packed_ref[...] = dot(held[...], w_ref[...]).astype(jnp.bfloat16)


def project(parts, gain, w):
    length = parts[0].shape[0] * SEQ
    return pl.pallas_call(
        project_kernel,
        in_specs=[VMEM] * (len(parts) + 2),
        out_specs=[VMEM] * 2,
        out_shape=[near_out((w.shape[0], length)), near_out((length, w.shape[1]))],
        scratch_shapes=[pltpu.VMEM((length, w.shape[0]), jnp.bfloat16)],
        compiler_params=within(24),
        name="project",
    )(*far(parts[0]), *far(*parts[1:]), *far(gain.reshape(1, -1), w))


def weights_kernel(*refs):
    parts, (q_ref, k_ref, o_ref) = refs[:SEQ], refs[SEQ:]
    factor = 1.0 / math.sqrt(HEAD_DIM)
    slots = parts[0].shape[0] - 8
    span = slots * SEQ
    keys = [p[:slots] for p in parts] + [k_ref[...]]
    flags = [
        jnp.concatenate([p[slots + r : slots + r + 1] for r in range(slots // HEAD_DIM)], axis=1)
        > 0.5
        for p in parts
    ]
    step = 128
    for r in range(q_ref.shape[0] // step):
        rows = slice(r * step, (r + 1) * step)
        query = q_ref[rows]
        scores = [dot(query, k, NT) * factor for k in keys]
        for n in range(SEQ):
            scores[n] = jnp.where(flags[n], scores[n], -1e30)
        top = jnp.max(scores[SEQ], axis=-1, keepdims=True)
        for n in range(SEQ):
            top = jnp.maximum(top, jnp.max(scores[n], axis=-1, keepdims=True))
        expo = [jnp.exp(s - top) for s in scores]
        total = sum(jnp.sum(e, axis=-1, keepdims=True) for e in expo)
        over = 1.0 / total
        for n in range(SEQ):
            o_ref[0, rows, n * slots : (n + 1) * slots] = (expo[n] * over).astype(jnp.bfloat16)
        o_ref[0, rows, span:] = (expo[SEQ] * over).astype(jnp.bfloat16)


def attention_weights(key_parts, packed):
    length = packed.shape[0]
    heads = key_parts[0].shape[1] // HEAD_DIM
    rows = key_parts[0].shape[0]
    total = (rows - 8) * SEQ + length
    part = pl.BlockSpec((rows, HEAD_DIM), lambda h: (0, h))
    return pl.pallas_call(
        weights_kernel,
        grid=(heads,),
        in_specs=[part] * SEQ
        + [pl.BlockSpec((length, HEAD_DIM), lambda h, j=j: (0, 3 * h + j)) for j in range(2)],
        out_specs=pl.BlockSpec((1, length, total), lambda h: (h, 0, 0)),
        out_shape=near_out((heads, length, total)),
        compiler_params=within(20),
        name="attention_weights",
    )(*far(*key_parts), *near(packed, packed))


def mix_kernel(*refs):
    w_ref, parts, v_ref, outs = refs[0], refs[1 : SEQ + 1], refs[SEQ + 1], refs[SEQ + 2 :]
    slots = parts[0].shape[0]
    count = outs[0].shape[0]
    mixed = dot(w_ref[0, :, slots * SEQ :], v_ref[...])
    for n in range(SEQ):
        mixed += dot(w_ref[0, :, n * slots : (n + 1) * slots], parts[n][...])
    mixed = mixed.astype(jnp.bfloat16)
    for n in range(SEQ):
        outs[n][...] = mixed[n * count : (n + 1) * count]


def attention_mix(weights, value_parts, packed):
    heads, length, total = weights.shape
    slots, features = value_parts[0].shape
    count = length // SEQ
    return pl.pallas_call(
        mix_kernel,
        grid=(heads,),
        in_specs=[pl.BlockSpec((1, length, total), lambda h: (h, 0, 0))]
        + [pl.BlockSpec((slots, HEAD_DIM), lambda h: (0, h))] * SEQ
        + [pl.BlockSpec((length, HEAD_DIM), lambda h: (0, 3 * h + 2))],
        out_specs=[pl.BlockSpec((count, HEAD_DIM), lambda h: (0, h))] * SEQ,
        out_shape=[far_out((count, features))] * SEQ,
        compiler_params=within(12),
        name="attention_mix",
    )(*near(weights), *far(*value_parts), *near(packed))


def in_terms(total, shape):
    row = lax.broadcasted_iota(jnp.int32, shape, 0)
    result = jnp.zeros(shape, jnp.float32)
    for n in range(3):
        term = total.astype(jnp.bfloat16).astype(jnp.float32)
        result = jnp.where(row == n, term, result)
        total = total - term
    return result.astype(jnp.bfloat16)


def unit_of(grads, entries):
    total = sum(g[-8:, :HEAD_DIM].astype(jnp.float32) for g in grads)
    total = jnp.sum(total, axis=0, keepdims=True)[:, :1]
    return 1.0 / (total / entries + 1e-06)


def middle_kernel(*refs):
    parts, refs = refs[:SEQ], refs[SEQ:]
    blend_ref, latents_ref, fresh_ref, real_gain_ref, fake_gain_ref, w_ref = refs[:6]
    clean_ref, gap_ref = refs[6:8]
    outs, (out_w, held, sems) = refs[8 : 8 + SEQ], refs[8 + SEQ :]
    width = parts[0].shape[1]

    for k in range(SEQ):
        j = place_in_seq(k)
        for c in range(SEQ):
            pltpu.make_async_copy(
                w_ref.at[0, :, c, :, pl.ds(pl.multiple_of(j * width, 128), width)],
                out_w.at[j, :, :, c * width : (c + 1) * width],
                sems.at[k],
            ).start()
    copies = [pltpu.make_async_copy(out_w.at[k], out_w.at[k], sems.at[k]) for k in range(SEQ)]
    for n in range(2):
        copies.append(pltpu.make_async_copy(w_ref.at[n + 1], held.at[n], sems.at[SEQ + n]))
        copies[-1].start()

    def block(k):
        rows = out_w[place_in_seq(k)]
        return rows.reshape(width, rows.shape[2])

    copies[0].wait()
    update = dot(parts[0][...], block(0))
    for k in range(1, SEQ):
        copies[k].wait()
        update += dot(parts[k][...], block(k))
    clean = (latents_ref[...].astype(jnp.float32) + update).astype(jnp.bfloat16)
    clean_ref[...] = clean
    clean_f = clean.astype(jnp.float32)
    noisy = (
        (blend_ref[0:1, 0:1] * clean_f + blend_ref[1:2, 0:1] * fresh_ref[...].astype(jnp.float32))
        .astype(jnp.bfloat16)
        .astype(jnp.float32)
    )
    scaled = noisy * lax.rsqrt(jnp.mean(noisy * noisy, axis=-1, keepdims=True) + 1e-06)
    gain_shape = (clean.shape[1], clean.shape[1])
    real_in = (scaled * real_gain_ref[...]).astype(jnp.bfloat16)
    fake_in = (scaled * fake_gain_ref[...]).astype(jnp.bfloat16)
    copies[SEQ].wait()
    pred_real = noisy + dot(real_in, held[0].reshape(gain_shape))
    total = jnp.sum(jnp.abs(clean_f - pred_real), axis=(0, 1), keepdims=True)
    copies[SEQ + 1].wait()
    pred_fake = noisy + dot(fake_in, held[1].reshape(gain_shape))
    gap = (pred_fake - pred_real).astype(jnp.bfloat16)
    gap_ref[...] = gap
    count = gap.shape[0]
    terms = in_terms(total, (8, width))
    for k in range(SEQ):
        outs[k][:count] = dot(gap, block(k), NT).astype(jnp.bfloat16)
        outs[k][count:] = terms


def middle(blend, parts, latents, fresh, gain_real, gain_fake, whole):
    count, width = latents.shape
    return pl.pallas_call(
        middle_kernel,
        in_specs=[VMEM] * (SEQ + 5) + [ANY],
        out_specs=[VMEM] * (2 + SEQ),
        out_shape=[far_out((count, width))] * 2
        + [near_out((count + 8, parts[0].shape[1]))] * SEQ,
        scratch_shapes=[
            pltpu.VMEM((SEQ, whole.shape[1], *whole.shape[3:]), jnp.bfloat16),
            pltpu.VMEM((2, *whole.shape[1:]), jnp.bfloat16),
            pltpu.SemaphoreType.DMA((SEQ + 2,)),
        ],
        compiler_params=within(30),
        name="middle",
    )(
        *far(*parts, blend, latents, fresh, gain_real.reshape(1, -1), gain_fake.reshape(1, -1)),
        *far(whole),
    )


def split_rows(held, send_ref, keep_ref):
    core = lax.rem(lax.axis_index("dp"), 2)
    pairs = PARTS // 2
    rows = held.shape[0] // PARTS

    @pl.loop(0, pairs)
    def _(n):
        at = pl.ds(pl.multiple_of(n * rows, 8), rows)
        other, own = (2 * n + 1 - core) * rows, (2 * n + core) * rows
        send_ref[at] = held[pl.ds(pl.multiple_of(other, 8), rows)].astype(jnp.bfloat16)
        keep_ref[at] = held[pl.ds(pl.multiple_of(own, 8), rows)].astype(jnp.bfloat16)


def backward_kernel(*refs):
    w_ref, turned_ref = refs[:2]
    grads, refs = refs[2 : SEQ + 2], refs[SEQ + 2 :]
    key_parts, value_parts, refs = refs[:SEQ], refs[SEQ : 2 * SEQ], refs[2 * SEQ :]
    q_ref, k_ref, v_ref, send_ref, keep_ref, dpacked, held = refs
    length, width = dpacked.shape[0], turned_ref.shape[0]
    unit = unit_of(grads, length * width)
    factor = 1.0 / math.sqrt(HEAD_DIM) * unit
    slots = value_parts[0].shape[0]
    span = slots * SEQ
    keys = [p[:slots] for p in key_parts] + [k_ref[...]]
    values = [p[...] for p in value_parts] + [v_ref[...]]
    count = length // SEQ
    dkey = jnp.zeros((HEAD_DIM, length), jnp.float32)
    dvalue = jnp.zeros((HEAD_DIM, length), jnp.float32)
    per = 2
    for r in range(SEQ // per):
        rows = slice(r * per * count, (r + 1) * per * count)
        dmixed = jnp.concatenate([g[:count] for g in grads[r * per : (r + 1) * per]], axis=0)
        weights = [w_ref[0, rows, n * slots : (n + 1) * slots] for n in range(SEQ)]
        weights.append(w_ref[0, rows, span:])
        dprobs = [dot(dmixed, v, NT) for v in values]
        inner = sum(
            jnp.sum(p.astype(jnp.float32) * d, axis=-1, keepdims=True)
            for p, d in zip(weights, dprobs)
        )
        dscores = [
            (p.astype(jnp.float32) * (d - inner) * factor).astype(jnp.bfloat16)
            for p, d in zip(weights, dprobs)
        ]
        dquery = sum(dot(d, k) for d, k in zip(dscores, keys))
        dpacked[rows, :HEAD_DIM] = dquery.astype(jnp.bfloat16)
        dkey += dot(q_ref[rows], dscores[SEQ], TN)
        dvalue += dot(dmixed, weights[SEQ], TN)
    dpacked[:, HEAD_DIM : 2 * HEAD_DIM] = dkey.astype(jnp.bfloat16).T
    dpacked[:, 2 * HEAD_DIM :] = (dvalue * unit).astype(jnp.bfloat16).T
    held[...] = dot(turned_ref[...], dpacked[...])
    split_rows(held, send_ref, keep_ref)


def backward(first, heads, weights, turned, grads, key_parts, value_parts, packed):
    length, total = weights.shape[1:]
    width = turned.shape[0]
    slots = value_parts[0].shape[0]
    part = lambda rows: pl.BlockSpec((rows, HEAD_DIM), lambda h: (0, first + h))
    half = pl.BlockSpec((width // 2, 3 * HEAD_DIM), lambda h: (0, h))
    return pl.pallas_call(
        backward_kernel,
        grid=(heads,),
        in_specs=[pl.BlockSpec((1, length, total), lambda h: (first + h, 0, 0))]
        + [pl.BlockSpec((width, length), lambda h: (0, 0))]
        + [part(grads[0].shape[0])] * SEQ
        + [part(key_parts[0].shape[0])] * SEQ
        + [part(slots)] * SEQ
        + [pl.BlockSpec((length, HEAD_DIM), lambda h, j=j: (0, 3 * (first + h) + j)) for j in range(3)],
        out_specs=[half] * 2,
        out_shape=[far_out((width // 2, heads * 3 * HEAD_DIM))] * 2,
        scratch_shapes=[
            pltpu.VMEM((length, 3 * HEAD_DIM), jnp.bfloat16),
            pltpu.VMEM((width, 3 * HEAD_DIM), jnp.float32),
        ],
        compiler_params=within(26),
        name="backward",
    )(
        *near(weights, turned, *grads),
        *far(*key_parts, *value_parts),
        *near(packed, packed, packed),
    )


def out_grad_kernel(*refs):
    grads, gaps, mixed = refs[:SEQ], refs[SEQ : 2 * SEQ], refs[2 * SEQ : 3 * SEQ]
    send_ref, keep_ref, held = refs[3 * SEQ :]
    total = dot(gaps[0][...], mixed[0][...], TN)
    for k in range(1, SEQ):
        total += dot(gaps[k][...], mixed[k][...], TN)
    entries = gaps[0].shape[0] * SEQ * gaps[0].shape[1]
    held[...] = total * unit_of(grads, entries)
    split_rows(held, send_ref, keep_ref)


def out_gradient(grads, gaps, mixed):
    width, features = gaps[0].shape[1], mixed[0].shape[1]
    return pl.pallas_call(
        out_grad_kernel,
        in_specs=[VMEM] * (3 * SEQ),
        out_specs=[VMEM] * 2,
        out_shape=[far_out((width // 2, features))] * 2,
        scratch_shapes=[pltpu.VMEM((width, features), jnp.float32)],
        compiler_params=within(16),
        name="out_gradient",
    )(*near(*grads), *far(*gaps, *mixed))


def swapped(x):
    return lax.ppermute(x, "dp", [(n, n ^ 1) for n in range(PARTS)])


def added(a, b):
    return (a.astype(jnp.float32) + b.astype(jnp.float32)).astype(jnp.bfloat16)


def summed_over_chips(x):
    pieces = x.reshape(PARTS // 2, x.shape[0] * 2 // PARTS, x.shape[1])
    arrived = lax.all_to_all(
        pieces, "dp", split_axis=0, concat_axis=0, tiled=True, axis_index_groups=chip_groups()
    )
    return arrived.astype(jnp.float32).sum(axis=0)


def shards(
    latents,
    fresh_noise,
    cache_key,
    cache_value,
    cache_frame,
    block_index,
    timestep,
    gain_gen,
    w_qkv,
    w_out,
    gain_real,
    w_real,
    gain_fake,
    w_fake,
):
    position = lax.axis_index("seq")
    replica = lax.axis_index("dp")
    latents, fresh_noise = latents[0], fresh_noise[0]
    cache_key, cache_value = cache_key[0], cache_value[0]
    count, width = latents.shape
    slots = cache_key.shape[0]
    features = w_out.shape[0]
    heads_here = features // HEAD_DIM

    slice_at = jnp.reshape((replica // 4) * 2 + replica % 2, (1,)).astype(jnp.int32)
    own = weight_slices(w_out, w_real, w_fake, slice_at, width // (PARTS // 2))
    parts = [own] + [shifted(own, -k) for k in range(1, SEQ)]
    slices = placed(parts)
    whole = lax.all_gather(slices, "dp", axis=1, tiled=True, axis_index_groups=plane_groups())
    whole = whole.reshape(3, PARTS // 2 // SEQ, SEQ, slices.shape[1], width)

    half = count // 2
    before, after = shifted(latents, 1), shifted(latents, -1)
    tokens = [latents, before, shifted(before[:half], 1), shifted(after[half:], -1), after]
    start = block_index[0] * FRAMES
    open_slots = (cache_frame >= start - WINDOW_FRAMES) & (cache_frame < start)
    flags = open_slots.astype(jnp.bfloat16).reshape(slots // HEAD_DIM, HEAD_DIM)
    flags = jnp.pad(jnp.tile(flags, (1, heads_here)), ((0, 8 - slots // HEAD_DIM), (0, 0)))

    def exchanged(make):
        return [make(position)] + [shifted(make(position + k), k) for k in range(1, SEQ)]

    key_parts = exchanged(lambda j: jnp.concatenate([block_of(cache_key, j, 1), flags], axis=0))
    value_parts = exchanged(lambda j: block_of(cache_value, j, 1))
    turned, packed = project(tokens, gain_gen, w_qkv)
    weights = attention_weights(key_parts, packed)
    mixed = attention_mix(weights, value_parts, packed)

    back = [mixed[0]] + [shifted(mixed[k], -k) for k in range(1, SEQ)]
    angle = math.pi / 2 * timestep.astype(jnp.float32) / 1000.0
    blend = jnp.broadcast_to(jnp.stack([jnp.cos(angle), jnp.sin(angle)]), (2, HEAD_DIM))
    clean, gap, *dmixed = middle(
        blend, back, latents, fresh_noise, gain_real, gain_fake, whole
    )
    grads = [dmixed[0]] + [shifted(dmixed[k], k) for k in range(1, SEQ)]
    gaps = [gap] + [shifted(gap, k) for k in range(1, SEQ)]
    sums = []
    for heads in (range(0, heads_here - 1), range(heads_here - 1, heads_here)):
        halves = backward(
            heads[0], len(heads), weights, turned, grads, key_parts, value_parts, packed
        )
        sums.append((swapped(halves[0]), halves[1]))
    halves = out_gradient(grads, gaps, mixed)
    sums.append((swapped(halves[0]), halves[1]))
    share_a = summed_over_chips(added(*sums[0]))
    share_b = summed_over_chips(
        added(*(jnp.concatenate([p, q], axis=1) for p, q in zip(sums[1], sums[2])))
    )
    rest = sums[1][0].shape[1]
    qkv_share = jnp.concatenate([share_a, share_b[:, :rest]], axis=1)
    return (clean[None], qkv_share, share_b[:, rest:].T)


def solution(mesh):
    in_specs = (
        P("dp", "seq", None),
        P("dp", "seq", None),
        P("dp", "seq", None),
        P("dp", "seq", None),
        P("dp", "seq"),
        P(),
        P("dp"),
        P(),
        P(None, "seq"),
        P("seq", None),
        P(),
        P(None, "seq"),
        P(),
        P(None, "seq"),
    )
    out_specs = (P("dp", "seq", None), P("dp", "seq"), P("seq", "dp"))

    return jax.shard_map(shards, mesh=mesh, in_specs=in_specs, out_specs=out_specs, check_vma=False)
```
